16 devices in a mesh: dp: 4 (over z, y), cp: 4 (over x, core).
Axes of the slice: x: 2, y: 2, z: 2, core: 2. Of those that a mesh axis runs over, the one named last changes fastest.
Arguments:
- hidden_in: bfloat16 [128, 768, 384], P('dp', 'cp'), parts along dimension 0
- pad_mask: int32 [128, 768], P('dp', 'cp'), parts along dimension 0
- d_out: bfloat16 [128, 768, 384], P('dp', 'cp'), parts along dimension 0
- g_attn: bfloat16 [2, 384], replicated
- g_mlp: bfloat16 [2, 384], replicated
- w_qkv: bfloat16 [2, 384, 1152], replicated
- w_out: bfloat16 [2, 384, 384], replicated
- w_in: bfloat16 [2, 384, 1152], replicated
- w_down: bfloat16 [2, 576, 384], replicated
Outputs:
- output 1: bfloat16 [128, 768, 384], P('dp', 'cp'), parts along dimension 0
- output 2: bfloat16 [128, 768, 384], P('dp', 'cp'), parts along dimension 0
- output 3: float32 [8, 384], P('dp'), parts along dimension 0
- output 4: float32 [8, 384], P('dp'), parts along dimension 0
- output 5: float32 [8, 384, 1152], P('dp'), parts along dimension 0
- output 6: float32 [8, 384, 384], P('dp'), parts along dimension 0
- output 7: float32 [8, 384, 1152], P('dp'), parts along dimension 0
- output 8: float32 [8, 576, 384], P('dp'), parts along dimension 0
There are 4 independent parts. The reference program is written for one: setup_inputs(seed, part) draws one part's arguments, and reference() takes and returns one part's arrays. A program takes and returns all parts, laid end to end along the dimension named above; an argument that names none is the same for every part.
All inputs are finite; a program needn't handle non-finite values.
Results may differ from the reference program's by a relative error of at most 0.02.
Values are sent between devices in bfloat16 or wider.
A program may use at most 1 GiB of HBM per device.

```python
import math
import jax
import jax.numpy as jnp
from jax import lax

BATCH = 32
SEQ = 768
DIM = 384
HEADS = 6
FFN = 576
HEAD_DIM = 64
WINDOW_HALF = 64
QUERY_BLOCK = 128
EPS = 1e-5
LOCAL_THETA = 10000.0
GLOBAL_THETA = 160000.0
NEG_BIG = -1e30
SCALE = HEAD_DIM ** -0.5


def setup_inputs(seed: int = 0, part: int = 0) -> dict:
    part_keys = jax.random.split(jax.random.fold_in(jax.random.key(seed), part), 3)
    shared_keys = jax.random.split(jax.random.key(seed + 1), 6)
    lengths = jax.random.randint(part_keys[1], (BATCH,), SEQ // 4, SEQ + 1)
    qk_gain = math.sqrt(0.8 * math.sqrt(math.log(SEQ)))
    col_scale = jnp.concatenate([jnp.full((2 * DIM,), qk_gain, jnp.float32), jnp.ones((DIM,), jnp.float32)])
    hidden_in = jax.random.normal(part_keys[0], (BATCH, SEQ, DIM), jnp.float32)
    d_out = jax.random.normal(part_keys[2], (BATCH, SEQ, DIM), jnp.float32)
    g_attn = 1.0 + 0.3 * jax.random.normal(shared_keys[0], (2, DIM), jnp.float32)
    g_mlp = 1.0 + 0.3 * jax.random.normal(shared_keys[1], (2, DIM), jnp.float32)
    w_qkv = jax.random.normal(shared_keys[2], (2, DIM, 3 * DIM), jnp.float32) * (DIM ** -0.5) * col_scale
    w_out = jax.random.normal(shared_keys[3], (2, DIM, DIM), jnp.float32) * (DIM ** -0.5)
    w_in = jax.random.normal(shared_keys[4], (2, DIM, 2 * FFN), jnp.float32) * (DIM ** -0.5)
    w_down = jax.random.normal(shared_keys[5], (2, FFN, DIM), jnp.float32) * (FFN ** -0.5)
    return {
        'hidden_in': hidden_in.astype(jnp.bfloat16),
        'pad_mask': (jnp.arange(SEQ)[None, :] < lengths[:, None]).astype(jnp.int32),
        'd_out': d_out.astype(jnp.bfloat16),
        'g_attn': g_attn.astype(jnp.bfloat16),
        'g_mlp': g_mlp.astype(jnp.bfloat16),
        'w_qkv': w_qkv.astype(jnp.bfloat16),
        'w_out': w_out.astype(jnp.bfloat16),
        'w_in': w_in.astype(jnp.bfloat16),
        'w_down': w_down.astype(jnp.bfloat16),
    }


def layer_norm(x_f, gain):
    centred = x_f - jnp.mean(x_f, axis=-1, keepdims=True)
    variance = jnp.mean(centred * centred, axis=-1, keepdims=True)
    return centred * lax.rsqrt(variance + EPS) * gain.astype(jnp.float32)


def project(act_bf, weight):
    flat_out = jnp.dot(act_bf.reshape(-1, act_bf.shape[-1]), weight, preferred_element_type=jnp.float32)
    return flat_out.reshape(act_bf.shape[:-1] + (weight.shape[-1],))


def rotary(heads_f, rope_theta):
    inv_freq = rope_theta ** (-jnp.arange(0, HEAD_DIM, 2, dtype=jnp.float32) / HEAD_DIM)
    angles = jnp.arange(SEQ, dtype=jnp.float32)[:, None] * inv_freq[None, :]
    angles = jnp.concatenate([angles, angles], axis=-1)
    first_half, second_half = jnp.split(heads_f, 2, axis=-1)
    turned = jnp.concatenate([-second_half, first_half], axis=-1)
    return heads_f * jnp.cos(angles)[:, None, :] + turned * jnp.sin(angles)[:, None, :]


def key_windows(ext_rows, n_blocks):
    win_span = n_blocks * WINDOW_HALF
    new_shape = (ext_rows.shape[0], n_blocks, WINDOW_HALF) + ext_rows.shape[2:]
    shifted_views = [ext_rows[:, shift_idx * WINDOW_HALF: shift_idx * WINDOW_HALF + win_span].reshape(new_shape) for shift_idx in range(3)]
    return jnp.concatenate(shifted_views, axis=2)


def local_attention(q_val, k_val, v_val, key_ok):
    n_blocks = SEQ // WINDOW_HALF
    widths = ((0, 0), (WINDOW_HALF, WINDOW_HALF), (0, 0), (0, 0))
    k_win = key_windows(jnp.pad(k_val.astype(jnp.float32), widths), n_blocks)
    v_win = key_windows(jnp.pad(v_val.astype(jnp.float32), widths), n_blocks)
    ok_win = key_windows(jnp.pad(key_ok, ((0, 0), (WINDOW_HALF, WINDOW_HALF))), n_blocks)
    q_blocks = q_val.astype(jnp.float32).reshape(BATCH, n_blocks, WINDOW_HALF, HEADS, HEAD_DIM)
    offset = jnp.arange(3 * WINDOW_HALF)[None, :] - WINDOW_HALF - jnp.arange(WINDOW_HALF)[:, None]
    allowed = (jnp.abs(offset) <= WINDOW_HALF) & (ok_win[:, :, None, :] | (offset == 0))
    scores = jnp.einsum('bnqhd,bnkhd->bnhqk', q_blocks, k_win) * SCALE
    scores = jnp.where(allowed[:, :, None], scores, NEG_BIG)
    prob_bf = jax.nn.softmax(scores, axis=-1).astype(jnp.bfloat16).astype(jnp.float32)
    mixed_out = jnp.einsum('bnhqk,bnkhd->bnqhd', prob_bf, v_win)
    return mixed_out.reshape(BATCH, SEQ, DIM).astype(jnp.bfloat16)


def global_attention(q_val, k_val, v_val, key_ok):
    k_f = k_val.astype(jnp.float32)
    v_f = v_val.astype(jnp.float32)

    def one_block(q_block):
        scores = jnp.einsum('bqhd,bkhd->bhqk', q_block.astype(jnp.float32), k_f) * SCALE
        scores = jnp.where(key_ok[:, None, None, :], scores, NEG_BIG)
        prob_bf = jax.nn.softmax(scores, axis=-1).astype(jnp.bfloat16).astype(jnp.float32)
        return jnp.einsum('bhqk,bkhd->bqhd', prob_bf, v_f).astype(jnp.bfloat16)

    q_blocks = jnp.moveaxis(q_val.reshape(BATCH, SEQ // QUERY_BLOCK, QUERY_BLOCK, HEADS, HEAD_DIM), 1, 0)
    mixed_out = lax.map(jax.checkpoint(one_block), q_blocks)
    return jnp.moveaxis(mixed_out, 0, 1).reshape(BATCH, SEQ, DIM)


def encoder_layer(x_val, layer_idx, weights, key_ok, is_global):
    g_attn, g_mlp, w_qkv, w_out, w_in, w_down = weights
    u_val = layer_norm(x_val.astype(jnp.float32), g_attn[layer_idx]).astype(jnp.bfloat16)
    qkv_f = project(u_val, w_qkv[layer_idx]).reshape(BATCH, SEQ, 3, HEADS, HEAD_DIM)
    rope_theta = GLOBAL_THETA if is_global else LOCAL_THETA
    q_val = rotary(qkv_f[:, :, 0], rope_theta).astype(jnp.bfloat16)
    k_val = rotary(qkv_f[:, :, 1], rope_theta).astype(jnp.bfloat16)
    v_val = qkv_f[:, :, 2].astype(jnp.bfloat16)
    if is_global:
        attn_out = global_attention(q_val, k_val, v_val, key_ok)
    else:
        attn_out = local_attention(q_val, k_val, v_val, key_ok)
    h_val = (x_val.astype(jnp.float32) + project(attn_out, w_out[layer_idx])).astype(jnp.bfloat16)
    u_mlp = layer_norm(h_val.astype(jnp.float32), g_mlp[layer_idx]).astype(jnp.bfloat16)
    mixed_in = project(u_mlp, w_in[layer_idx])
    act_bf = (jax.nn.gelu(mixed_in[..., :FFN], approximate=False) * mixed_in[..., FFN:]).astype(jnp.bfloat16)
    return (h_val.astype(jnp.float32) + project(act_bf, w_down[layer_idx])).astype(jnp.bfloat16)


def reference(hidden_in, pad_mask, d_out, g_attn, g_mlp, w_qkv, w_out, w_in, w_down):
    key_ok = pad_mask > 0

    def forward(x_in, weights):
        hidden_mid = encoder_layer(x_in, 0, weights, key_ok, False)
        return encoder_layer(hidden_mid, 1, weights, key_ok, True)

    hidden_out, pullback = jax.vjp(forward, hidden_in, (g_attn, g_mlp, w_qkv, w_out, w_in, w_down))
    d_hidden, weight_grads = pullback(d_out)
    return (hidden_out, d_hidden, weight_grads[0].astype(jnp.float32), weight_grads[1].astype(jnp.float32),
            weight_grads[2].astype(jnp.float32), weight_grads[3].astype(jnp.float32),
            weight_grads[4].astype(jnp.float32), weight_grads[5].astype(jnp.float32))
```

```python
import numpy as np
import jax
import jax.numpy as jnp
from jax import lax
from jax.experimental import pallas as pl
from jax.experimental.pallas import tpu as pltpu
from jax.sharding import PartitionSpec as P

HEADS = 6
HD = 64
WIN = 64
EPS = 1e-5
THETAS = (10000.0, 160000.0)
NEG = -1e30
SEQ = 768
DIM = 384
FFN = 576
CH = 256
NCH = SEQ // CH
F32 = jnp.float32
BF16 = jnp.bfloat16
KEYS = (((0, 384), (128, 640), (384, 768)), ((0, 768),) * 3)


def rope_tables():
    out = np.zeros((2, 2, HD // 2, SEQ), np.float32)
    pos = np.arange(SEQ, dtype=np.float32)
    for l, theta in enumerate(THETAS):
        freq = np.float32(theta) ** (-np.arange(0, HD, 2, dtype=np.float32) / np.float32(HD))
        ang = (pos[None, :] * freq.astype(np.float32)[:, None]).astype(np.float32).astype(np.float64)
        out[l, 0] = np.cos(ang)
        out[l, 1] = np.sin(ang)
    return out


def nn(a, b):
    return jnp.dot(a, b, preferred_element_type=F32)


def nt(a, b):
    return lax.dot_general(a, b, (((1,), (1,)), ((), ())), preferred_element_type=F32)


def wide(g):
    return jnp.concatenate([g] * (CH // 128), axis=1)


def fold(z):
    return sum(z[:, i * 128:(i + 1) * 128] for i in range(1, CH // 128)) + z[:, :128]


def ln_fwd(z, gain, st, row, sl):
    mean = jnp.sum(z, axis=0, keepdims=True) * (1.0 / DIM)
    c = z - mean
    var = jnp.sum(c * c, axis=0, keepdims=True) * (1.0 / DIM)
    r = lax.rsqrt(var + EPS)
    st[row:row + 1, sl] = mean
    st[row + 1:row + 2, sl] = r
    return (c * r * wide(gain)).astype(BF16)


def ln_bwd(z, du, gain, st, row, sl):
    mean = st[row:row + 1, sl]
    r = st[row + 1:row + 2, sl]
    xhat = (z - mean) * r
    dg = fold(du * xhat)
    gw = wide(gain)
    dxh = du * gw
    m1 = jnp.sum(dxh, axis=0, keepdims=True) * (1.0 / DIM)
    m2 = jnp.sum(dxh * xhat, axis=0, keepdims=True) * (1.0 / DIM)
    return r * (dxh - m1 - xhat * m2), dg, (xhat * gw).astype(BF16)


def turn(z, cos, sin):
    n = z.shape[0] // HD
    z4 = z.reshape(n, 2, HD // 2, z.shape[1])
    a, b = z4[:, 0], z4[:, 1]
    return jnp.stack([a * cos - b * sin, b * cos + a * sin], axis=1).reshape(z.shape)


def gelu_parts(a):
    cdf = 0.5 * (1.0 + lax.erf(a * (2.0 ** -0.5)))
    return a * cdf, cdf


class Bufs:
    pass


def forward(l, b, write_y):
    st = b.st.at[l]
    for c in range(NCH):
        sl = pl.ds(c * CH, CH)
        u = ln_fwd(b.xT[l, :, sl].astype(F32), b.g[0, l], st, 0, sl)
        z = nn(b.wTqkv[l], u)
        cos, sin = b.rope[l, 0, :, sl], b.rope[l, 1, :, sl]
        b.qkvT[l, :DIM, sl] = turn(z[:DIM], cos * 0.125, sin * 0.125).astype(BF16)
        b.qkvT[l, DIM:2 * DIM, sl] = turn(z[DIM:2 * DIM], cos, sin).astype(BF16)
        b.qkvT[l, 2 * DIM:, sl] = z[2 * DIM:].astype(BF16)

    def head(h):
        row = pl.multiple_of(h * HD, HD)
        kT = b.qkvT[l, pl.ds(DIM + row, HD), :]
        vT = b.qkvT[l, pl.ds(2 * DIM + row, HD), :]
        if l == 0:
            kn = kT.T
        else:
            kn = jnp.concatenate([kT, b.kextra[...]], axis=0).T
        for c in range(NCH):
            sl = pl.ds(c * CH, CH)
            k0, k1 = KEYS[l][c]
            qT = b.qkvT[l, pl.ds(row, HD), sl]
            if l == 0:
                s = nn(kn[k0:k1], qT) + b.bias[c, :k1 - k0, :].astype(F32)
            else:
                s = nn(kn, jnp.concatenate([qT, b.qextra[...]], axis=0))
            m = jnp.max(s, axis=0, keepdims=True)
            e = jnp.exp(s - m)
            p = (e * (1.0 / jnp.sum(e, axis=0, keepdims=True))).astype(BF16)
            if l == 0:
                b.p0[h, c, :k1 - k0, :] = p
            else:
                b.p1[h, :, sl] = p
            b.oT[l, pl.ds(row, HD), sl] = nn(vT[:, k0:k1], p).astype(BF16)

    def pair(i, carry):
        head(2 * i)
        head(2 * i + 1)
        return carry
    lax.fori_loop(0, HEADS // 2, pair, 0)

    for c in range(NCH):
        sl = pl.ds(c * CH, CH)
        hb = (b.xT[l, :, sl].astype(F32) + nn(b.wTout[l], b.oT[l, :, sl])).astype(BF16)
        b.hT[l, :, sl] = hb
        u2 = ln_fwd(hb.astype(F32), b.g[1, l], st, 2, sl)
        mix = nn(b.wTin[l], u2)
        b.mixT[l, :, sl] = mix
        act = (gelu_parts(mix[:FFN])[0] * mix[FFN:]).astype(BF16)
        y = (hb.astype(F32) + nn(b.wTdown[l], act)).astype(BF16)
        write_y(c, sl, y)


def backward(l, b, read_dy, write_dx):
    st = b.st.at[l]
    for c in range(NCH):
        sl = pl.ds(c * CH, CH)
        dy = read_dy(c, sl)
        dyb = dy.astype(BF16)
        b.dybT[:, sl] = dyb
        dact = nn(b.wdown[l], dyb)
        a, g = b.mixT[l, :FFN, sl], b.mixT[l, FFN:, sl]
        ge, cdf = gelu_parts(a)
        b.actT[:, sl] = (ge * g).astype(BF16)
        pdf = jnp.exp(a * a * -0.5) * 0.3989422804014327
        b.dbigT[:FFN, sl] = (dact * g * (cdf + a * pdf)).astype(BF16)
        b.dbigT[FFN:, sl] = (dact * ge).astype(BF16)
        du = nn(b.win[l], b.dbigT[:, sl])
        dn, dg, b.uT[:, sl] = ln_bwd(b.hT[l, :, sl].astype(F32), du, b.g[1, l], st, 2, sl)
        b.dg[1, l] += dg
        dh = dy + dn
        b.dyT[:, sl] = dh
        dhb = dh.astype(BF16)
        b.dhbT[:, sl] = dhb
        b.doT[:, sl] = nn(b.wout[l], dhb).astype(BF16)
    b.adown[l] += nt(b.actT[...], b.dybT[...])
    b.ain[l] += nt(b.uT[...], b.dbigT[...])
    b.aout[l] += nt(b.oT[l], b.dhbT[...])

    def head(h):
        row = pl.multiple_of(h * HD, HD)
        qT = b.qkvT[l, pl.ds(row, HD), :]
        kT = b.qkvT[l, pl.ds(DIM + row, HD), :]
        vn = b.qkvT[l, pl.ds(2 * DIM + row, HD), :].T
        doT = b.doT[pl.ds(row, HD), :]
        prod = doT.astype(F32) * b.oT[l, pl.ds(row, HD), :].astype(F32)
        delta = jnp.sum(prod, axis=0, keepdims=True)
        dq, dk, dv = [], [None] * 6, [None] * 6
        if l == 1:
            dvT = nt(doT, b.p1[h])
        for c in range(NCH):
            cs = slice(c * CH, (c + 1) * CH)
            sl = pl.ds(c * CH, CH)
            k0, k1 = KEYS[l][c]
            p = b.p0[h, c, :k1 - k0, :] if l == 0 else b.p1[h, :, sl]
            dp = nn(vn[k0:k1], doT[:, cs])
            ds = (p.astype(F32) * (dp - delta[:, cs])).astype(BF16)
            dq.append(nn(kT[:, k0:k1], ds) * 0.125)
            if l == 1:
                b.p1[h, :, sl] = ds
            else:
                dkc, dvc = nt(qT[:, cs], ds), nt(doT[:, cs], p)
                for j in range(k0 // 128, k1 // 128):
                    js = slice(j * 128 - k0, (j + 1) * 128 - k0)
                    dk[j] = dkc[:, js] if dk[j] is None else dk[j] + dkc[:, js]
                    dv[j] = dvc[:, js] if dv[j] is None else dv[j] + dvc[:, js]
        if l == 1:
            dkT = nt(qT, b.p1[h])
        else:
            dkT, dvT = jnp.concatenate(dk, axis=1), jnp.concatenate(dv, axis=1)
        dqT = jnp.concatenate(dq, axis=1)
        cos, sin = b.rope[l, 0], -b.rope[l, 1]
        b.dbigT[pl.ds(row, HD), :] = turn(dqT, cos, sin).astype(BF16)
        b.dbigT[pl.ds(DIM + row, HD), :] = turn(dkT, cos, sin).astype(BF16)
        b.dbigT[pl.ds(2 * DIM + row, HD), :] = dvT.astype(BF16)

    def pair(i, carry):
        head(2 * i)
        head(2 * i + 1)
        return carry
    lax.fori_loop(0, HEADS // 2, pair, 0)

    for c in range(NCH):
        sl = pl.ds(c * CH, CH)
        du = nn(b.wqkv[l], b.dbigT[:, sl])
        dn, dg, b.uT[:, sl] = ln_bwd(b.xT[l, :, sl].astype(F32), du, b.g[0, l], st, 0, sl)
        b.dg[0, l] += dg
        write_dx(c, sl, b.dyT[:, sl] + dn)
    b.aqkv[l] += nt(b.uT[...], b.dbigT[...])


def start_up(b):
    for src, dst in ((b.wqkv, b.wTqkv), (b.wout, b.wTout), (b.win, b.wTin), (b.wdown, b.wTdown)):
        for l in range(2):
            dst[l] = src[l].T
    for acc in (b.aqkv, b.aout, b.ain, b.adown, b.dg):
        acc[...] = jnp.zeros_like(acc)
    row0 = lax.broadcasted_iota(jnp.int32, (HD, CH), 0) == 0
    b.qextra[...] = jnp.where(row0, 1.0, 0.0).astype(BF16)


def masks(b, pad):
    ok = pad > 0
    row0 = lax.broadcasted_iota(jnp.int32, (HD, SEQ), 0) == 0
    b.kextra[...] = jnp.where(row0 & jnp.logical_not(ok), NEG, 0.0).astype(BF16)
    okc = jnp.broadcast_to(jnp.where(ok, 1.0, 0.0), (128, SEQ)).T
    for c in range(NCH):
        k0, k1 = KEYS[0][c]
        shape = (k1 - k0, CH)
        off = lax.broadcasted_iota(jnp.int32, shape, 0) + (k0 - c * CH) - lax.broadcasted_iota(jnp.int32, shape, 1)
        near = (jnp.abs(off) <= WIN) & (wide(okc[k0:k1]) > 0.5)
        b.bias[c, :k1 - k0, :] = jnp.where(near | (off == 0), 0.0, NEG).astype(BF16)


NAMES = ('wTqkv', 'wTout', 'wTin', 'wTdown', 'aqkv', 'aout', 'ain', 'adown', 'dg', 'st', 'xT', 'uT', 'qkvT',
         'p0', 'p1', 'oT', 'hT', 'mixT', 'actT', 'dyT', 'dybT', 'dbigT', 'dhbT', 'doT', 'bias',
         'kextra', 'qextra')


def scratch():
    v = pltpu.VMEM
    return [v((2, 3 * DIM, DIM), BF16), v((2, DIM, DIM), BF16), v((2, 2 * FFN, DIM), BF16), v((2, DIM, FFN), BF16),
            v((2, DIM, 3 * DIM), F32), v((2, DIM, DIM), F32), v((2, DIM, 2 * FFN), F32), v((2, FFN, DIM), F32),
            v((2, 2, DIM, 128), F32), v((2, 8, SEQ), F32),
            v((2, DIM, SEQ), BF16), v((DIM, SEQ), BF16), v((2, 3 * DIM, SEQ), BF16),
            v((HEADS, NCH, 512, CH), BF16), v((HEADS, SEQ, SEQ), BF16),
            v((2, DIM, SEQ), BF16), v((2, DIM, SEQ), BF16), v((2, 2 * FFN, SEQ), F32),
            v((FFN, SEQ), BF16), v((DIM, SEQ), F32), v((DIM, SEQ), BF16), v((3 * DIM, SEQ), BF16),
            v((DIM, SEQ), BF16), v((DIM, SEQ), BF16), v((NCH, 512, CH), BF16),
            v((HD, SEQ), BF16), v((HD, CH), BF16)]


def kernel(x_ref, dout_ref, pad_ref, g_ref, rope_ref, wqkv, wout, win, wdown,
           y_ref, dx_ref, oqkv, oout, oin, odown, odg, *refs):
    b = Bufs()
    for name, ref in zip(NAMES, refs):
        setattr(b, name, ref)
    b.g, b.rope, b.wqkv, b.wout, b.win, b.wdown = g_ref, rope_ref, wqkv, wout, win, wdown
    step = pl.program_id(0)

    @pl.when(step == 0)
    def _():
        start_up(b)

    masks(b, pad_ref[0])
    b.xT[0] = x_ref[0].T

    def keep(c, sl, y):
        b.xT[1, :, sl] = y

    def put_y(c, sl, y):
        y_ref[0, sl, :] = y.T

    def get_dout(c, sl):
        return dout_ref[0, sl, :].T.astype(F32)

    def put_d(c, sl, d):
        b.dyT[:, sl] = d

    def get_d(c, sl):
        return b.dyT[:, sl]

    def put_dx(c, sl, d):
        dx_ref[0, sl, :] = d.astype(BF16).T

    forward(0, b, keep)
    forward(1, b, put_y)
    backward(1, b, get_dout, put_d)
    backward(0, b, get_d, put_dx)

    @pl.when(step == pl.num_programs(0) - 1)
    def _():
        for src, dst in ((b.aqkv, oqkv), (b.aout, oout), (b.ain, oin), (b.adown, odown), (b.dg, odg)):
            pltpu.sync_copy(src, dst)


def run_kernel(x, dout, pad, g, rope, w_qkv, w_out, w_in, w_down):
    n = x.shape[0]
    per_seq = pl.BlockSpec((1, SEQ, DIM), lambda i: (i, 0, 0))

    def whole(a):
        return pl.BlockSpec(a.shape, lambda i: (0,) * a.ndim, pipeline_mode=pl.Buffered(1))
    any_spec = pl.BlockSpec(memory_space=pl.ANY)
    outs = [jax.ShapeDtypeStruct((n, SEQ, DIM), BF16)] * 2 + [
        jax.ShapeDtypeStruct(s, F32) for s in ((2, DIM, 3 * DIM), (2, DIM, DIM), (2, DIM, 2 * FFN), (2, FFN, DIM), (2, 2, DIM, 128))]
    return pl.pallas_call(
        kernel, grid=(n,), out_shape=outs,
        in_specs=[per_seq, per_seq, pl.BlockSpec((1, 1, SEQ), lambda i: (i, 0, 0)), whole(g), whole(rope),
                  whole(w_qkv), whole(w_out), whole(w_in), whole(w_down)],
        out_specs=[per_seq, per_seq] + [any_spec] * 5,
        scratch_shapes=scratch(),
        compiler_params=pltpu.CompilerParams(dimension_semantics=("arbitrary",), vmem_limit_bytes=67043328),
    )(x, dout, pad, g, rope, w_qkv, w_out, w_in, w_down)


def solution(mesh):
    act_spec = P('dp', 'cp', None)

    def device_pass(x_loc, pad_loc, dout_loc, g_attn, g_mlp, w_qkv, w_out, w_in, w_down):
        x = lax.all_to_all(x_loc, 'cp', 0, 1, tiled=True)
        dout = lax.all_to_all(dout_loc, 'cp', 0, 1, tiled=True)
        pad = lax.all_to_all(pad_loc, 'cp', 0, 1, tiled=True)
        g = jnp.broadcast_to(jnp.stack([g_attn, g_mlp]).astype(F32)[..., None], (2, 2, DIM, 128))
        y, dx, dqkv, dout_w, din, ddown, dg = run_kernel(
            x, dout, pad[:, None, :], g, jnp.asarray(rope_tables()), w_qkv, w_out, w_in, w_down)
        y = lax.all_to_all(y, 'cp', 1, 0, tiled=True)
        dx = lax.all_to_all(dx, 'cp', 1, 0, tiled=True)
        dg = jnp.sum(dg, axis=-1)
        sums = lax.psum((dg[0], dg[1], dqkv, dout_w, din, ddown), 'cp')
        return (y, dx) + tuple(sums)

    return jax.shard_map(device_pass, mesh=mesh,
                         in_specs=(act_spec, P('dp', 'cp'), act_spec, P(), P(), P(), P(), P(), P()),
                         out_specs=(act_spec, act_spec, P('dp'), P('dp'), P('dp'), P('dp'), P('dp'), P('dp')),
                         check_vma=False)
```

```python
import numpy as np
import jax
import jax.numpy as jnp
from jax import lax
from jax.experimental import pallas as pl
from jax.experimental.pallas import tpu as pltpu
from jax.sharding import PartitionSpec as P

HEADS = 6
HD = 64
WIN = 64
EPS = 1e-5
THETAS = (10000.0, 160000.0)
NEG = -1e30
SEQ = 768
DIM = 384
FFN = 576
CH = 256
NCH = SEQ // CH
F32 = jnp.float32
BF16 = jnp.bfloat16
KEYS = (((0, 384), (128, 640), (384, 768)), ((0, 768),) * 3)


def rope_tables():
    out = np.zeros((2, 2, HD // 2, SEQ), np.float32)
    pos = np.arange(SEQ, dtype=np.float32)
    for l, theta in enumerate(THETAS):
        freq = np.float32(theta) ** (-np.arange(0, HD, 2, dtype=np.float32) / np.float32(HD))
        ang = (pos[None, :] * freq.astype(np.float32)[:, None]).astype(np.float32).astype(np.float64)
        out[l, 0] = np.cos(ang)
        out[l, 1] = np.sin(ang)
    return out


def nn(a, b):
    return jnp.dot(a, b, preferred_element_type=F32)


def nt(a, b):
    return lax.dot_general(a, b, (((1,), (1,)), ((), ())), preferred_element_type=F32)


def wide(g):
    return jnp.concatenate([g] * (CH // 128), axis=1)


def fold(z):
    return sum(z[:, i * 128:(i + 1) * 128] for i in range(1, CH // 128)) + z[:, :128]


def ln_fwd(z, gain, st, row, sl):
    mean = jnp.sum(z, axis=0, keepdims=True) * (1.0 / DIM)
    c = z - mean
    var = jnp.sum(c * c, axis=0, keepdims=True) * (1.0 / DIM)
    r = lax.rsqrt(var + EPS)
    st[row:row + 1, sl] = mean
    st[row + 1:row + 2, sl] = r
    return (c * r * wide(gain)).astype(BF16)


def ln_bwd(z, du, gain, st, row, sl):
    mean = st[row:row + 1, sl]
    r = st[row + 1:row + 2, sl]
    xhat = (z - mean) * r
    dg = fold(du * xhat)
    gw = wide(gain)
    dxh = du * gw
    m1 = jnp.sum(dxh, axis=0, keepdims=True) * (1.0 / DIM)
    m2 = jnp.sum(dxh * xhat, axis=0, keepdims=True) * (1.0 / DIM)
    return r * (dxh - m1 - xhat * m2), dg, (xhat * gw).astype(BF16)


def turn(z, cos, sin):
    n = z.shape[0] // HD
    z4 = z.reshape(n, 2, HD // 2, z.shape[1])
    a, b = z4[:, 0], z4[:, 1]
    return jnp.stack([a * cos - b * sin, b * cos + a * sin], axis=1).reshape(z.shape)


def gelu_parts(a):
    cdf = 0.5 * (1.0 + lax.erf(a * (2.0 ** -0.5)))
    return a * cdf, cdf


class Bufs:
    pass


def forward(l, b, write_y):
    st = b.st.at[l]
    for c in range(NCH):
        sl = pl.ds(c * CH, CH)
        u = ln_fwd(b.xT[l, :, sl].astype(F32), b.g[0, l], st, 0, sl)
        z = nn(b.wTqkv[l], u)
        cos, sin = b.rope[l, 0, :, sl], b.rope[l, 1, :, sl]
        b.qkvT[l, :DIM, sl] = turn(z[:DIM], cos * 0.125, sin * 0.125).astype(BF16)
        b.qkvT[l, DIM:2 * DIM, sl] = turn(z[DIM:2 * DIM], cos, sin).astype(BF16)
        b.qkvT[l, 2 * DIM:, sl] = z[2 * DIM:].astype(BF16)

    def head(h):
        row = pl.multiple_of(h * HD, HD)
        kT = b.qkvT[l, pl.ds(DIM + row, HD), :]
        vT = b.qkvT[l, pl.ds(2 * DIM + row, HD), :]
        if l == 0:
            kn = kT.T
        else:
            kn = jnp.concatenate([kT, b.kextra[...]], axis=0).T
        for c in range(NCH):
            sl = pl.ds(c * CH, CH)
            k0, k1 = KEYS[l][c]
            qT = b.qkvT[l, pl.ds(row, HD), sl]
            if l == 0:
                s = nn(kn[k0:k1], qT) + b.bias[c, :k1 - k0, :].astype(F32)
            else:
                s = nn(kn, jnp.concatenate([qT, b.qextra[...]], axis=0))
            m = jnp.max(s, axis=0, keepdims=True)
            e = jnp.exp(s - m)
            p = (e * (1.0 / jnp.sum(e, axis=0, keepdims=True))).astype(BF16)
            if l == 0:
                b.p0[h, c, :k1 - k0, :] = p
            else:
                b.p1[h, :, sl] = p
            b.oT[l, pl.ds(row, HD), sl] = nn(vT[:, k0:k1], p).astype(BF16)

    def pair(i, carry):
        head(2 * i)
        head(2 * i + 1)
        return carry
    lax.fori_loop(0, HEADS // 2, pair, 0)

    for c in range(NCH):
        sl = pl.ds(c * CH, CH)
        hb = (b.xT[l, :, sl].astype(F32) + nn(b.wTout[l], b.oT[l, :, sl])).astype(BF16)
        b.hT[l, :, sl] = hb
        u2 = ln_fwd(hb.astype(F32), b.g[1, l], st, 2, sl)
        mix = nn(b.wTin[l], u2)
        b.mixT[l, :, sl] = mix
        act = (gelu_parts(mix[:FFN])[0] * mix[FFN:]).astype(BF16)
        y = (hb.astype(F32) + nn(b.wTdown[l], act)).astype(BF16)
        write_y(c, sl, y)


def backward(l, b, read_dy, write_dx):
    st = b.st.at[l]
    for c in range(NCH):
        sl = pl.ds(c * CH, CH)
        dy = read_dy(c, sl)
        dyb = dy.astype(BF16)
        b.dybT[:, sl] = dyb
        dact = nn(b.wdown[l], dyb)
        a, g = b.mixT[l, :FFN, sl], b.mixT[l, FFN:, sl]
        ge, cdf = gelu_parts(a)
        b.actT[:, sl] = (ge * g).astype(BF16)
        pdf = jnp.exp(a * a * -0.5) * 0.3989422804014327
        b.dbigT[:FFN, sl] = (dact * g * (cdf + a * pdf)).astype(BF16)
        b.dbigT[FFN:, sl] = (dact * ge).astype(BF16)
        du = nn(b.win[l], b.dbigT[:, sl])
        dn, dg, b.uT[:, sl] = ln_bwd(b.hT[l, :, sl].astype(F32), du, b.g[1, l], st, 2, sl)
        b.dg[1, l] += dg
        dh = dy + dn
        b.dyT[:, sl] = dh
        dhb = dh.astype(BF16)
        b.dhbT[:, sl] = dhb
        b.doT[:, sl] = nn(b.wout[l], dhb).astype(BF16)
    b.adown[l] += nt(b.actT[...], b.dybT[...])
    b.ain[l] += nt(b.uT[...], b.dbigT[...])
    b.aout[l] += nt(b.oT[l], b.dhbT[...])

    def head(h):
        row = pl.multiple_of(h * HD, HD)
        qT = b.qkvT[l, pl.ds(row, HD), :]
        kT = b.qkvT[l, pl.ds(DIM + row, HD), :]
        vn = b.qkvT[l, pl.ds(2 * DIM + row, HD), :].T
        doT = b.doT[pl.ds(row, HD), :]
        prod = doT.astype(F32) * b.oT[l, pl.ds(row, HD), :].astype(F32)
        delta = jnp.sum(prod, axis=0, keepdims=True)
        dq, dk, dv = [], [None] * 6, [None] * 6
        if l == 1:
            dvT = nt(doT, b.p1[h])
        for c in range(NCH):
            cs = slice(c * CH, (c + 1) * CH)
            sl = pl.ds(c * CH, CH)
            k0, k1 = KEYS[l][c]
            p = b.p0[h, c, :k1 - k0, :] if l == 0 else b.p1[h, :, sl]
            dp = nn(vn[k0:k1], doT[:, cs])
            ds = (p.astype(F32) * (dp - delta[:, cs])).astype(BF16)
            dq.append(nn(kT[:, k0:k1], ds) * 0.125)
            if l == 1:
                b.p1[h, :, sl] = ds
            else:
                dkc, dvc = nt(qT[:, cs], ds), nt(doT[:, cs], p)
                for j in range(k0 // 128, k1 // 128):
                    js = slice(j * 128 - k0, (j + 1) * 128 - k0)
                    dk[j] = dkc[:, js] if dk[j] is None else dk[j] + dkc[:, js]
                    dv[j] = dvc[:, js] if dv[j] is None else dv[j] + dvc[:, js]
        if l == 1:
            dkT = nt(qT, b.p1[h])
        else:
            dkT, dvT = jnp.concatenate(dk, axis=1), jnp.concatenate(dv, axis=1)
        dqT = jnp.concatenate(dq, axis=1)
        cos, sin = b.rope[l, 0], -b.rope[l, 1]
        b.dbigT[pl.ds(row, HD), :] = turn(dqT, cos, sin).astype(BF16)
        b.dbigT[pl.ds(DIM + row, HD), :] = turn(dkT, cos, sin).astype(BF16)
        b.dbigT[pl.ds(2 * DIM + row, HD), :] = dvT.astype(BF16)

    def pair(i, carry):
        head(2 * i)
        head(2 * i + 1)
        return carry
    lax.fori_loop(0, HEADS // 2, pair, 0)

    for c in range(NCH):
        sl = pl.ds(c * CH, CH)
        du = nn(b.wqkv[l], b.dbigT[:, sl])
        dn, dg, b.uT[:, sl] = ln_bwd(b.xT[l, :, sl].astype(F32), du, b.g[0, l], st, 0, sl)
        b.dg[0, l] += dg
        write_dx(c, sl, b.dyT[:, sl] + dn)
    b.aqkv[l] += nt(b.uT[...], b.dbigT[...])


def start_up(b):
    for src, dst in ((b.wqkv, b.wTqkv), (b.wout, b.wTout), (b.win, b.wTin), (b.wdown, b.wTdown)):
        for l in range(2):
            dst[l] = src[l].T
    for acc in (b.aqkv, b.aout, b.ain, b.adown, b.dg):
        acc[...] = jnp.zeros_like(acc)
    row0 = lax.broadcasted_iota(jnp.int32, (HD, CH), 0) == 0
    b.qextra[...] = jnp.where(row0, 1.0, 0.0).astype(BF16)


def masks(b, pad):
    ok = pad > 0
    row0 = lax.broadcasted_iota(jnp.int32, (HD, SEQ), 0) == 0
    b.kextra[...] = jnp.where(row0 & jnp.logical_not(ok), NEG, 0.0).astype(BF16)
    okc = jnp.broadcast_to(jnp.where(ok, 1.0, 0.0), (128, SEQ)).T
    for c in range(NCH):
        k0, k1 = KEYS[0][c]
        shape = (k1 - k0, CH)
        off = lax.broadcasted_iota(jnp.int32, shape, 0) + (k0 - c * CH) - lax.broadcasted_iota(jnp.int32, shape, 1)
        near = (jnp.abs(off) <= WIN) & (wide(okc[k0:k1]) > 0.5)
        b.bias[c, :k1 - k0, :] = jnp.where(near | (off == 0), 0.0, NEG).astype(BF16)


NAMES = ('wTqkv', 'wTout', 'wTin', 'wTdown', 'aqkv', 'aout', 'ain', 'adown', 'dg', 'st', 'xT', 'uT', 'qkvT',
         'p0', 'p1', 'oT', 'hT', 'mixT', 'actT', 'dyT', 'dybT', 'dbigT', 'dhbT', 'doT', 'bias',
         'kextra', 'qextra', 'xbuf', 'dbuf', 'ybuf', 'dxbuf', 'padin', 'padrow', 'dgs', 'dgl', 'dgb', 'dgr',
         'in_send', 'in_recv', 'pad_send', 'pad_recv', 'fetch', 'out_send', 'out_recv', 'own', 'ready',
         'g_send', 'g_recv', 'g_own')

N_CP = 4
PER = 8
PIECE = SEQ // N_CP
GROUPS = ((0, 1), (1, 1), (2, 2), (4, 4))
ISSUE = (0, 0, 1, 2)
BLOCKS = tuple([('aqkv', 0, DIM, i * DIM) for i in range(3)] + [('ain', 0, DIM, i * DIM) for i in range(3)]
               + [('aout', 0, DIM, 0), ('adown', 0, DIM, 0), ('adown', DIM, FFN - DIM, 0)])


def scratch():
    v = pltpu.VMEM
    dma, reg = pltpu.SemaphoreType.DMA, pltpu.SemaphoreType.REGULAR
    n_g = len(BLOCKS) + 1
    return [v((2, 3 * DIM, DIM), BF16), v((2, DIM, DIM), BF16), v((2, 2 * FFN, DIM), BF16), v((2, DIM, FFN), BF16),
            v((2, DIM, 3 * DIM), F32), v((2, DIM, DIM), F32), v((2, DIM, 2 * FFN), F32), v((2, FFN, DIM), F32),
            v((2, 2, DIM, 128), F32), v((2, 8, SEQ), F32),
            v((2, DIM, SEQ), BF16), v((DIM, SEQ), BF16), v((2, 3 * DIM, SEQ), BF16),
            v((HEADS, NCH, 512, CH), BF16), v((HEADS, SEQ, SEQ), BF16),
            v((2, DIM, SEQ), BF16), v((2, DIM, SEQ), BF16), v((2, 2 * FFN, SEQ), F32),
            v((FFN, SEQ), BF16), v((DIM, SEQ), F32), v((DIM, SEQ), BF16), v((3 * DIM, SEQ), BF16),
            v((DIM, SEQ), BF16), v((DIM, SEQ), BF16), v((NCH, 512, CH), BF16),
            v((HD, SEQ), BF16), v((HD, CH), BF16),
            v((SEQ, DIM), BF16), v((SEQ, DIM), BF16), v((SEQ, DIM), BF16), v((SEQ, DIM), BF16),
            v((N_CP, PER, PIECE), jnp.int32), v((8, SEQ), jnp.int32),
            v((2, 16, DIM), F32), v((16, DIM), F32), v((16, DIM), BF16), v((16, DIM), BF16),
            dma((2, 3)), dma((2, len(GROUPS), 3)), dma((3,)), dma((3,)), dma((3, N_CP)),
            dma((2, 3)), dma((2, 3)), dma((2,)), reg((2,)),
            dma((3, n_g)), dma((3, n_g)), dma((n_g,))]


def rows(j):
    return pl.ds(pl.multiple_of(j * PIECE, 64), PIECE)


def kernel(x_loc, dout_loc, pad_loc, g_ref, rope_ref, wqkv, wout, win, wdown,
           y_out, dx_out, oqkv, oout, oin, odown, odg, xland, dland, *refs):
    b = Bufs()
    for name, ref in zip(NAMES, refs):
        setattr(b, name, ref)
    b.g, b.rope, b.wqkv, b.wout, b.win, b.wdown = g_ref, rope_ref, wqkv, wout, win, wdown
    me = lax.axis_index('cp')
    core = lax.rem(me, 2)
    mate = me + 1 - 2 * core
    across = lax.rem(me + 2, N_CP)

    def far(d):
        return lax.rem(me + d, N_CP)

    def near(d):
        return lax.rem(me + N_CP - d, N_CP)

    def remote(src, dst, ssem, rsem, j):
        return pltpu.make_async_remote_copy(src_ref=src, dst_ref=dst, send_sem=ssem, recv_sem=rsem,
                                            device_id={'cp': j}, device_id_type=pl.DeviceIdType.MESH)

    ins = ((x_loc, xland), (dout_loc, dland))
    outs = ((b.ybuf, y_out), (b.dxbuf, dx_out))

    def send_in(a, gi, d):
        first, n = GROUPS[gi]
        src, land = ins[a]
        return remote(src.at[pl.ds(far(d) * PER + first, n)], land.at[d - 1, pl.ds(first, n)],
                      b.in_send.at[a, d - 1], b.in_recv.at[a, gi, d - 1], far(d))

    def issue(gi):
        for a in range(2):
            for d in (2, 1, 3):
                send_in(a, gi, d).start()

    def arrived(a, gi):
        for d in (1, 2, 3):
            send_in(a, gi, d).wait_recv()

    def fetches(a, s):
        src, land = ins[a]
        buf = (b.xbuf, b.dbuf)[a]
        res = [pltpu.make_async_copy(src.at[me * PER + s], buf.at[rows(me)], b.fetch.at[a, 0])]
        for d in (1, 2, 3):
            res.append(pltpu.make_async_copy(land.at[d - 1, s], buf.at[rows(near(d))], b.fetch.at[a, d]))
        return res

    def out_copies(a, s):
        buf, out = outs[a]
        res = [remote(buf.at[rows(far(d))], out.at[me * PER + s], b.out_send.at[a, d - 1], b.out_recv.at[a, d - 1], far(d))
               for d in (2, 1, 3)]
        return res, pltpu.make_async_copy(buf.at[rows(me)], out.at[me * PER + s], b.own.at[a])

    def send_out(a, s):
        res, own = out_copies(a, s)
        for c in res:
            c.start()
        own.start()

    def drain_out(a, s):
        res, own = out_copies(a, s)
        for c in res:
            c.wait_send()
        own.wait()

    def pad_copies():
        return [remote(pad_loc.at[pl.ds(pl.multiple_of(far(d) * PER, PER), PER)], b.padin.at[d], b.pad_send.at[d - 1],
                       b.pad_recv.at[d - 1], far(d)) for d in (1, 2, 3)]

    barrier = pltpu.get_barrier_semaphore()
    for d in (1, 2, 3):
        pl.semaphore_signal(barrier, inc=1, device_id={'cp': far(d)}, device_id_type=pl.DeviceIdType.MESH)
    pl.semaphore_wait(barrier, 3)
    for c in pad_copies():
        c.start()
    pad_own = pltpu.make_async_copy(pad_loc.at[pl.ds(pl.multiple_of(me * PER, PER), PER)], b.padin.at[0], b.fetch.at[2, 0])
    pad_own.start()
    for gi in range(len(GROUPS)):
        if ISSUE[gi] == 0:
            issue(gi)
    start_up(b)
    pad_own.wait()
    for c in pad_copies():
        c.wait_recv()
    arrived(0, 0)
    for c in fetches(0, 0):
        c.start()

    def keep(c, sl, y):
        b.xT[1, :, sl] = y

    def put_y(c, sl, y):
        b.ybuf[sl, :] = y.T

    def get_dout(c, sl):
        return b.dbuf[sl, :].T.astype(F32)

    def put_d(c, sl, d):
        b.dyT[:, sl] = d

    def get_d(c, sl):
        return b.dyT[:, sl]

    def put_dx(c, sl, d):
        b.dxbuf[sl, :] = d.astype(BF16).T

    def step(s, carry):
        for gi in range(len(GROUPS)):
            if ISSUE[gi] > 0:
                @pl.when(s == ISSUE[gi])
                def _():
                    issue(gi)
        for j in range(N_CP):
            d = lax.rem(me + N_CP - j, N_CP)
            b.padrow[0:1, j * PIECE:(j + 1) * PIECE] = b.padin[d, pl.ds(s, 1), :]
        masks(b, b.padrow[0:1, :])
        for c in fetches(0, s):
            c.wait()
        b.xT[0] = b.xbuf[...].T
        forward(0, b, keep)
        for gi in range(len(GROUPS)):
            @pl.when(s == GROUPS[gi][0])
            def _():
                arrived(1, gi)
        for c in fetches(1, s):
            c.start()

        @pl.when(s > 0)
        def _():
            drain_out(0, s)
        forward(1, b, put_y)
        send_out(0, s)
        for c in fetches(1, s):
            c.wait()
        backward(1, b, get_dout, put_d)
        for gi in range(1, len(GROUPS)):
            @pl.when(s + 1 == GROUPS[gi][0])
            def _():
                arrived(0, gi)

        @pl.when(s + 1 < PER)
        def _():
            for c in fetches(0, s + 1):
                c.start()

        @pl.when(s > 0)
        def _():
            drain_out(1, s)
        backward(0, b, get_d, put_dx)
        send_out(1, s)
        return carry
    lax.fori_loop(0, PER, step, 0)

    for l in range(2):
        for k in range(2):
            b.dgs[l, k:k + 1, :] = jnp.sum(b.dg[k, l].T, axis=0, keepdims=True)
        b.dgs[l, 2:, :] = jnp.zeros((14, DIM), F32)
    for i, j in enumerate((mate, across)):
        pl.semaphore_signal(b.ready.at[i], inc=1, device_id={'cp': j}, device_id_type=pl.DeviceIdType.MESH)

    grads = {'aqkv': oqkv, 'aout': oout, 'ain': oin, 'adown': odown}

    def tile(ref, i, n):
        return ref.at[i // 6 if ref is b.mixT else i // 4,
                      pl.ds((i % 6 // 2 if ref is b.mixT else i % 4 // 2) * DIM, n), pl.ds(i % 2 * DIM, DIM)]

    def places(i):
        if i == len(BLOCKS):
            return (lambda l: b.dgs.at[l]), b.dgl, b.dgb, b.dgr, (lambda l: odg.at[l])
        name, r0, n, c0 = BLOCKS[i]
        acc, out = getattr(b, name), grads[name]
        return ((lambda l: acc.at[l, pl.ds(r0, n), pl.ds(c0, DIM)]), tile(b.mixT, i, n), tile(b.p1, i, n),
                tile(b.p1, i + 12, n), (lambda l: out.at[l, pl.ds(r0, n), pl.ds(c0, DIM)]))

    n_g = len(BLOCKS) + 1

    def first(i):
        acc, land, _, _, _ = places(i)
        return remote(acc(1 - core), land, b.g_send.at[0, i], b.g_recv.at[0, i], mate)

    def second(i):
        _, _, out, land, _ = places(i)
        return remote(out, land, b.g_send.at[1, i], b.g_recv.at[1, i], across)

    def third(i):
        acc, _, _, _, out = places(i)
        return (remote(acc(core), out(core), b.g_send.at[2, i], b.g_recv.at[2, i], mate),
                pltpu.make_async_copy(acc(core), out(core), b.g_own.at[i]))

    pl.semaphore_wait(b.ready.at[0], 1)
    for i in range(n_g):
        first(i).start()
    pl.semaphore_wait(b.ready.at[1], 1)
    for i in range(n_g):
        acc, land, out, _, _ = places(i)
        first(i).wait_recv()
        out[...] = (acc(core)[...] + land[...]).astype(BF16)
        second(i).start()
    for i in range(n_g):
        acc, _, mine, land, _ = places(i)
        second(i).wait_recv()
        acc(core)[...] = mine[...].astype(F32) + land[...].astype(F32)
        for c in third(i):
            c.start()
    for i in range(n_g):
        first(i).wait_send()
        second(i).wait_send()
        third(i)[0].wait()
        third(i)[1].wait()
    for c in pad_copies():
        c.wait_send()
    for a in range(2):
        drain_out(a, PER - 1)
        src = ins[a][0]
        buf, out = outs[a]
        for d in (1, 2, 3):
            whole_in = src.at[pl.ds(far(d) * PER, PER)]
            remote(whole_in, whole_in, b.in_send.at[a, d - 1], b.in_send.at[a, d - 1], far(d)).wait_send()
            whole_out = out.at[pl.ds(near(d) * PER, PER)]
            remote(whole_out, whole_out, b.out_recv.at[a, d - 1], b.out_recv.at[a, d - 1], near(d)).wait_recv()


def run_kernel(x, dout, pad, g, rope, w_qkv, w_out, w_in, w_down):
    any_spec = pl.BlockSpec(memory_space=pl.ANY)
    vm = pl.BlockSpec(memory_space=pltpu.VMEM)
    sds = jax.ShapeDtypeStruct
    outs = [sds(x.shape, BF16)] * 2 + [
        sds(s, F32) for s in ((2, DIM, 3 * DIM), (2, DIM, DIM), (2, DIM, 2 * FFN), (2, FFN, DIM), (2, 16, DIM))] + [
        sds((3, PER, PIECE, DIM), BF16)] * 2
    return pl.pallas_call(
        kernel, out_shape=outs,
        in_specs=[any_spec] * 3 + [vm] * 6,
        out_specs=[any_spec] * 9,
        scratch_shapes=scratch(),
        compiler_params=pltpu.CompilerParams(vmem_limit_bytes=67043328, collective_id=0, has_side_effects=True),
    )(x, dout, pad, g, rope, w_qkv, w_out, w_in, w_down)


def solution(mesh):
    act_spec = P('dp', 'cp', None)

    def device_pass(x_loc, pad_loc, dout_loc, g_attn, g_mlp, w_qkv, w_out, w_in, w_down):
        g = jnp.broadcast_to(jnp.stack([g_attn, g_mlp]).astype(F32)[..., None], (2, 2, DIM, 128))
        y, dx, dqkv, dout_w, din, ddown, dg = run_kernel(
            x_loc, dout_loc, pad_loc, g, jnp.asarray(rope_tables()), w_qkv, w_out, w_in, w_down)[:7]
        return y, dx, dg[:, 0], dg[:, 1], dqkv, dout_w, din, ddown

    return jax.shard_map(device_pass, mesh=mesh,
                         in_specs=(act_spec, P('dp', 'cp'), act_spec, P(), P(), P(), P(), P(), P()),
                         out_specs=(act_spec, act_spec, P('dp'), P('dp'), P('dp'), P('dp'), P('dp'), P('dp')),
                         check_vma=False)
```

```python
import numpy as np
import jax
import jax.numpy as jnp
from jax import lax
from jax.experimental import pallas as pl
from jax.experimental.pallas import tpu as pltpu
from jax.sharding import PartitionSpec as P

HEADS = 6
HD = 64
WIN = 64
EPS = 1e-5
THETAS = (10000.0, 160000.0)
NEG = -1e30
SEQ = 768
DIM = 384
FFN = 576
CH = 256
NCH = SEQ // CH
F32 = jnp.float32
BF16 = jnp.bfloat16
KEYS = (((0, 384), (128, 640), (384, 768)), ((0, 768),) * 3)


def rope_tables():
    out = np.zeros((2, 2, HD // 2, SEQ), np.float32)
    pos = np.arange(SEQ, dtype=np.float32)
    for l, theta in enumerate(THETAS):
        freq = np.float32(theta) ** (-np.arange(0, HD, 2, dtype=np.float32) / np.float32(HD))
        ang = (pos[None, :] * freq.astype(np.float32)[:, None]).astype(np.float32).astype(np.float64)
        out[l, 0] = np.cos(ang)
        out[l, 1] = np.sin(ang)
    return out


def nn(a, b):
    return jnp.dot(a, b, preferred_element_type=F32)


def nt(a, b):
    return lax.dot_general(a, b, (((1,), (1,)), ((), ())), preferred_element_type=F32)


def wide(g):
    return jnp.concatenate([g] * (CH // 128), axis=1)


def fold(z):
    return sum(z[:, i * 128:(i + 1) * 128] for i in range(1, CH // 128)) + z[:, :128]


def ln_fwd(z, gain, st, row, sl):
    mean = jnp.sum(z, axis=0, keepdims=True) * (1.0 / DIM)
    c = z - mean
    var = jnp.sum(c * c, axis=0, keepdims=True) * (1.0 / DIM)
    r = lax.rsqrt(var + EPS)
    st[row:row + 1, sl] = mean
    st[row + 1:row + 2, sl] = r
    return (c * r * wide(gain)).astype(BF16)


def ln_bwd(z, du, gain, st, row, sl):
    mean = st[row:row + 1, sl]
    r = st[row + 1:row + 2, sl]
    xhat = (z - mean) * r
    dg = fold(du * xhat)
    gw = wide(gain)
    dxh = du * gw
    m1 = jnp.sum(dxh, axis=0, keepdims=True) * (1.0 / DIM)
    m2 = jnp.sum(dxh * xhat, axis=0, keepdims=True) * (1.0 / DIM)
    return r * (dxh - m1 - xhat * m2), dg, (xhat * gw).astype(BF16)


def turn(z, cos, sin):
    n = z.shape[0] // HD
    z4 = z.reshape(n, 2, HD // 2, z.shape[1])
    a, b = z4[:, 0], z4[:, 1]
    return jnp.stack([a * cos - b * sin, b * cos + a * sin], axis=1).reshape(z.shape)


def gelu_parts(a):
    cdf = 0.5 * (1.0 + lax.erf(a * (2.0 ** -0.5)))
    return a * cdf, cdf


class Bufs:
    pass


def forward(l, b, write_y):
    st = b.st.at[l]
    tmp = {}

    def norm_in(c):
        sl = pl.ds(c * CH, CH)
        tmp['z', c] = nn(b.wTqkv[l], ln_fwd(b.xT[l, :, sl].astype(F32), b.g[0, l], st, 0, sl))

    def rotate(c):
        sl = pl.ds(c * CH, CH)
        z = tmp.pop(('z', c))
        cos, sin = b.rope[l, 0, :, sl], b.rope[l, 1, :, sl]
        b.qkvT[l, :DIM, sl] = turn(z[:DIM], cos * 0.125, sin * 0.125).astype(BF16)
        b.qkvT[l, DIM:2 * DIM, sl] = turn(z[DIM:2 * DIM], cos, sin).astype(BF16)
        b.qkvT[l, 2 * DIM:, sl] = z[2 * DIM:].astype(BF16)

    norm_in(0)
    norm_in(1)
    rotate(0)
    norm_in(2)
    rotate(1)
    rotate(2)

    def group(i, carry):
        heads = [2 * i, 2 * i + 1]
        rows_of = [pl.multiple_of(h * HD, HD) for h in heads]
        keys = []
        for row in rows_of:
            kT = b.qkvT[l, pl.ds(DIM + row, HD), :]
            keys.append(kT.T if l == 0 else jnp.concatenate([kT, b.kextra[...]], axis=0).T)

        def score(n):
            k, c = divmod(n, NCH)
            k0, k1 = KEYS[l][c]
            qT = b.qkvT[l, pl.ds(rows_of[k], HD), pl.ds(c * CH, CH)]
            if l == 0:
                return nn(keys[k][k0:k1], qT) + b.bias[c, :k1 - k0, :].astype(F32)
            return nn(keys[k], jnp.concatenate([qT, b.qextra[...]], axis=0))

        total = len(heads) * NCH
        s = score(0)
        for n in range(total):
            k, c = divmod(n, NCH)
            sl = pl.ds(c * CH, CH)
            k0, k1 = KEYS[l][c]
            later = score(n + 1) if n + 1 < total else None
            m = jnp.max(s, axis=0, keepdims=True)
            e = jnp.exp(s - m)
            p = (e * (1.0 / jnp.sum(e, axis=0, keepdims=True))).astype(BF16)
            if l == 0:
                b.p0[heads[k], c, :k1 - k0, :] = p
            else:
                b.p1[heads[k], :, sl] = p
            vT = b.qkvT[l, pl.ds(2 * DIM + rows_of[k], HD), k0:k1]
            b.oT[l, pl.ds(rows_of[k], HD), sl] = nn(vT, p).astype(BF16)
            s = later
        return carry
    lax.fori_loop(0, HEADS // 2, group, 0)

    def open_mlp(c):
        sl = pl.ds(c * CH, CH)
        hb = (b.xT[l, :, sl].astype(F32) + nn(b.wTout[l], b.oT[l, :, sl])).astype(BF16)
        b.hT[l, :, sl] = hb
        b.mixT[l, :, sl] = nn(b.wTin[l], ln_fwd(hb.astype(F32), b.g[1, l], st, 2, sl))

    def close_mlp(c):
        sl = pl.ds(c * CH, CH)
        act = (gelu_parts(b.mixT[l, :FFN, sl])[0] * b.mixT[l, FFN:, sl]).astype(BF16)
        write_y(c, sl, (b.hT[l, :, sl].astype(F32) + nn(b.wTdown[l], act)).astype(BF16))

    open_mlp(0)
    open_mlp(1)
    close_mlp(0)
    open_mlp(2)
    close_mlp(1)
    close_mlp(2)


def backward(l, b, read_dy, write_dx):
    st = b.st.at[l]
    tmp = {}

    def gate(c):
        sl = pl.ds(c * CH, CH)
        dyb = read_dy(c, sl).astype(BF16)
        b.dybT[:, sl] = dyb
        tmp['act', c] = nn(b.wdown[l], dyb)

    def ungate(c):
        sl = pl.ds(c * CH, CH)
        dact = tmp.pop(('act', c))
        a, g = b.mixT[l, :FFN, sl], b.mixT[l, FFN:, sl]
        ge, cdf = gelu_parts(a)
        b.actT[:, sl] = (ge * g).astype(BF16)
        pdf = jnp.exp(a * a * -0.5) * 0.3989422804014327
        b.dbigT[:FFN, sl] = (dact * g * (cdf + a * pdf)).astype(BF16)
        b.dbigT[FFN:, sl] = (dact * ge).astype(BF16)
        tmp['du', c] = nn(b.win[l], b.dbigT[:, sl])

    def unnorm(c):
        sl = pl.ds(c * CH, CH)
        dn, dg, b.uT[:, sl] = ln_bwd(b.hT[l, :, sl].astype(F32), tmp.pop(('du', c)), b.g[1, l], st, 2, sl)
        b.dg[1, l] += dg
        dh = read_dy(c, sl) + dn
        b.dyT[:, sl] = dh
        dhb = dh.astype(BF16)
        b.dhbT[:, sl] = dhb
        b.doT[:, sl] = nn(b.wout[l], dhb).astype(BF16)

    gate(0)
    gate(1)
    ungate(0)
    gate(2)
    ungate(1)
    unnorm(0)
    ungate(2)
    unnorm(1)
    b.adown[l] += nt(b.actT[...], b.dybT[...])
    unnorm(2)
    b.ain[l] += nt(b.uT[...], b.dbigT[...])
    b.aout[l] += nt(b.oT[l], b.dhbT[...])

    def group(i, carry):
        heads = [2 * i, 2 * i + 1]
        info = []
        for h in heads:
            row = pl.multiple_of(h * HD, HD)
            doT = b.doT[pl.ds(row, HD), :]
            prod = doT.astype(F32) * b.oT[l, pl.ds(row, HD), :].astype(F32)
            info.append((h, row, b.qkvT[l, pl.ds(row, HD), :], b.qkvT[l, pl.ds(DIM + row, HD), :],
                         b.qkvT[l, pl.ds(2 * DIM + row, HD), :].T, doT, jnp.sum(prod, axis=0, keepdims=True)))

        def dprob(n):
            k, c = divmod(n, NCH)
            k0, k1 = KEYS[l][c]
            return nn(info[k][4][k0:k1], info[k][5][:, c * CH:(c + 1) * CH])

        cos, sin = b.rope[l, 0], -b.rope[l, 1]
        total = len(heads) * NCH
        dp = dprob(0)
        for n in range(total):
            k, c = divmod(n, NCH)
            h, row, qT, kT, _, doT, delta = info[k]
            if c == 0:
                dq, dk, dv = [], [None] * 6, [None] * 6
                if l == 1:
                    dvT = nt(doT, b.p1[h])
            cs = slice(c * CH, (c + 1) * CH)
            sl = pl.ds(c * CH, CH)
            k0, k1 = KEYS[l][c]
            later = dprob(n + 1) if n + 1 < total else None
            p = b.p0[h, c, :k1 - k0, :] if l == 0 else b.p1[h, :, sl]
            ds = (p.astype(F32) * (dp - delta[:, cs])).astype(BF16)
            dp = later
            dq.append(nn(kT[:, k0:k1], ds) * 0.125)
            if l == 1:
                b.p1[h, :, sl] = ds
            else:
                dkc, dvc = nt(qT[:, cs], ds), nt(doT[:, cs], p)
                for j in range(k0 // 128, k1 // 128):
                    js = slice(j * 128 - k0, (j + 1) * 128 - k0)
                    dk[j] = dkc[:, js] if dk[j] is None else dk[j] + dkc[:, js]
                    dv[j] = dvc[:, js] if dv[j] is None else dv[j] + dvc[:, js]
            if c < NCH - 1:
                continue
            if l == 1:
                dkT = nt(qT, b.p1[h])
            else:
                dkT, dvT = jnp.concatenate(dk, axis=1), jnp.concatenate(dv, axis=1)
            b.dbigT[pl.ds(row, HD), :] = turn(jnp.concatenate(dq, axis=1), cos, sin).astype(BF16)
            b.dbigT[pl.ds(DIM + row, HD), :] = turn(dkT, cos, sin).astype(BF16)
            b.dbigT[pl.ds(2 * DIM + row, HD), :] = dvT.astype(BF16)
        return carry
    lax.fori_loop(0, HEADS // 2, group, 0)

    def unproject(c):
        tmp['du', c] = nn(b.wqkv[l], b.dbigT[:, pl.ds(c * CH, CH)])

    def finish(c):
        sl = pl.ds(c * CH, CH)
        dn, dg, b.uT[:, sl] = ln_bwd(b.xT[l, :, sl].astype(F32), tmp.pop(('du', c)), b.g[0, l], st, 0, sl)
        b.dg[0, l] += dg
        write_dx(c, sl, b.dyT[:, sl] + dn)

    unproject(0)
    unproject(1)
    finish(0)
    unproject(2)
    finish(1)
    finish(2)
    b.aqkv[l] += nt(b.uT[...], b.dbigT[...])


def start_up(b):
    for src, dst in ((b.wqkv, b.wTqkv), (b.wout, b.wTout), (b.win, b.wTin), (b.wdown, b.wTdown)):
        for l in range(2):
            dst[l] = src[l].T
    for acc in (b.aqkv, b.aout, b.ain, b.adown, b.dg):
        acc[...] = jnp.zeros_like(acc)
    row0 = lax.broadcasted_iota(jnp.int32, (HD, CH), 0) == 0
    b.qextra[...] = jnp.where(row0, 1.0, 0.0).astype(BF16)


def masks(b, pad):
    ok = pad > 0
    row0 = lax.broadcasted_iota(jnp.int32, (HD, SEQ), 0) == 0
    b.kextra[...] = jnp.where(row0 & jnp.logical_not(ok), NEG, 0.0).astype(BF16)
    okc = jnp.broadcast_to(jnp.where(ok, 1.0, 0.0), (128, SEQ)).T
    for c in range(NCH):
        k0, k1 = KEYS[0][c]
        shape = (k1 - k0, CH)
        off = lax.broadcasted_iota(jnp.int32, shape, 0) + (k0 - c * CH) - lax.broadcasted_iota(jnp.int32, shape, 1)
        near = (jnp.abs(off) <= WIN) & (wide(okc[k0:k1]) > 0.5)
        b.bias[c, :k1 - k0, :] = jnp.where(near | (off == 0), 0.0, NEG).astype(BF16)


NAMES = ('wTqkv', 'wTout', 'wTin', 'wTdown', 'aqkv', 'aout', 'ain', 'adown', 'dg', 'st', 'xT', 'uT', 'qkvT',
         'p0', 'p1', 'oT', 'hT', 'mixT', 'actT', 'dyT', 'dybT', 'dbigT', 'dhbT', 'doT', 'bias',
         'kextra', 'qextra', 'xbuf', 'dbuf', 'ybuf', 'dxbuf', 'padin', 'padrow', 'dgs', 'dgl', 'dgb', 'dgr',
         'in_send', 'in_recv', 'pad_send', 'pad_recv', 'fetch', 'out_send', 'out_recv', 'own', 'ready',
         'g_send', 'g_recv', 'g_own')

N_CP = 4
PER = 8
PIECE = SEQ // N_CP
GROUPS = ((0, 1), (1, 1), (2, 2), (4, 4))
ISSUE = (0, 0, 1, 2)
BLOCKS = tuple([('aqkv', 0, DIM, i * DIM) for i in range(3)] + [('ain', 0, DIM, i * DIM) for i in range(3)]
               + [('aout', 0, DIM, 0), ('adown', 0, DIM, 0), ('adown', DIM, FFN - DIM, 0)])


def scratch():
    v = pltpu.VMEM
    dma, reg = pltpu.SemaphoreType.DMA, pltpu.SemaphoreType.REGULAR
    n_g = len(BLOCKS) + 1
    return [v((2, 3 * DIM, DIM), BF16), v((2, DIM, DIM), BF16), v((2, 2 * FFN, DIM), BF16), v((2, DIM, FFN), BF16),
            v((2, DIM, 3 * DIM), F32), v((2, DIM, DIM), F32), v((2, DIM, 2 * FFN), F32), v((2, FFN, DIM), F32),
            v((2, 2, DIM, 128), F32), v((2, 8, SEQ), F32),
            v((2, DIM, SEQ), BF16), v((DIM, SEQ), BF16), v((2, 3 * DIM, SEQ), BF16),
            v((HEADS, NCH, 512, CH), BF16), v((HEADS, SEQ, SEQ), BF16),
            v((2, DIM, SEQ), BF16), v((2, DIM, SEQ), BF16), v((2, 2 * FFN, SEQ), F32),
            v((FFN, SEQ), BF16), v((DIM, SEQ), F32), v((DIM, SEQ), BF16), v((3 * DIM, SEQ), BF16),
            v((DIM, SEQ), BF16), v((DIM, SEQ), BF16), v((NCH, 512, CH), BF16),
            v((HD, SEQ), BF16), v((HD, CH), BF16),
            v((SEQ, DIM), BF16), v((SEQ, DIM), BF16), v((SEQ, DIM), BF16), v((SEQ, DIM), BF16),
            v((N_CP, PER, PIECE), jnp.int32), v((8, SEQ), jnp.int32),
            v((2, 16, DIM), F32), v((16, DIM), F32), v((16, DIM), BF16), v((16, DIM), BF16),
            dma((2, 3)), dma((2, len(GROUPS), 3)), dma((3,)), dma((3,)), dma((3, N_CP)),
            dma((2, 3)), dma((2, 3)), dma((2,)), reg((2,)),
            dma((3, n_g)), dma((3, n_g)), dma((n_g,))]


def rows(j):
    return pl.ds(pl.multiple_of(j * PIECE, 64), PIECE)


def kernel(x_loc, dout_loc, pad_loc, g_ref, rope_ref, wqkv, wout, win, wdown,
           y_out, dx_out, oqkv, oout, oin, odown, odg, xland, dland, *refs):
    b = Bufs()
    for name, ref in zip(NAMES, refs):
        setattr(b, name, ref)
    b.g, b.rope, b.wqkv, b.wout, b.win, b.wdown = g_ref, rope_ref, wqkv, wout, win, wdown
    me = lax.axis_index('cp')
    core = lax.rem(me, 2)
    mate = me + 1 - 2 * core
    across = lax.rem(me + 2, N_CP)

    def far(d):
        return lax.rem(me + d, N_CP)

    def near(d):
        return lax.rem(me + N_CP - d, N_CP)

    def remote(src, dst, ssem, rsem, j):
        return pltpu.make_async_remote_copy(src_ref=src, dst_ref=dst, send_sem=ssem, recv_sem=rsem,
                                            device_id={'cp': j}, device_id_type=pl.DeviceIdType.MESH)

    ins = ((x_loc, xland), (dout_loc, dland))
    outs = ((b.ybuf, y_out), (b.dxbuf, dx_out))

    def send_in(a, gi, d):
        first, n = GROUPS[gi]
        src, land = ins[a]
        return remote(src.at[pl.ds(far(d) * PER + first, n)], land.at[d - 1, pl.ds(first, n)],
                      b.in_send.at[a, d - 1], b.in_recv.at[a, gi, d - 1], far(d))

    def issue(gi):
        for a in range(2):
            for d in (2, 1, 3):
                send_in(a, gi, d).start()

    def arrived(a, gi):
        for d in (1, 2, 3):
            send_in(a, gi, d).wait_recv()

    def fetches(a, s):
        src, land = ins[a]
        buf = (b.xbuf, b.dbuf)[a]
        res = [pltpu.make_async_copy(src.at[me * PER + s], buf.at[rows(me)], b.fetch.at[a, 0])]
        for d in (1, 2, 3):
            res.append(pltpu.make_async_copy(land.at[d - 1, s], buf.at[rows(near(d))], b.fetch.at[a, d]))
        return res

    def out_copies(a, s):
        buf, out = outs[a]
        res = [remote(buf.at[rows(far(d))], out.at[me * PER + s], b.out_send.at[a, d - 1], b.out_recv.at[a, d - 1], far(d))
               for d in (2, 1, 3)]
        return res, pltpu.make_async_copy(buf.at[rows(me)], out.at[me * PER + s], b.own.at[a])

    def send_out(a, s):
        res, own = out_copies(a, s)
        for c in res:
            c.start()
        own.start()

    def drain_out(a, s):
        res, own = out_copies(a, s)
        for c in res:
            c.wait_send()
        own.wait()

    def pad_copies():
        return [remote(pad_loc.at[pl.ds(pl.multiple_of(far(d) * PER, PER), PER)], b.padin.at[d], b.pad_send.at[d - 1],
                       b.pad_recv.at[d - 1], far(d)) for d in (1, 2, 3)]

    barrier = pltpu.get_barrier_semaphore()
    for d in (1, 2, 3):
        pl.semaphore_signal(barrier, inc=1, device_id={'cp': far(d)}, device_id_type=pl.DeviceIdType.MESH)
    pl.semaphore_wait(barrier, 3)
    for c in pad_copies():
        c.start()
    pad_own = pltpu.make_async_copy(pad_loc.at[pl.ds(pl.multiple_of(me * PER, PER), PER)], b.padin.at[0], b.fetch.at[2, 0])
    pad_own.start()
    for gi in range(len(GROUPS)):
        if ISSUE[gi] == 0:
            issue(gi)
    start_up(b)
    pad_own.wait()
    for c in pad_copies():
        c.wait_recv()
    arrived(0, 0)
    for c in fetches(0, 0):
        c.start()

    def keep(c, sl, y):
        b.xT[1, :, sl] = y

    def put_y(c, sl, y):
        b.ybuf[sl, :] = y.T

    def get_dout(c, sl):
        return b.dbuf[sl, :].T.astype(F32)

    def put_d(c, sl, d):
        b.dyT[:, sl] = d

    def get_d(c, sl):
        return b.dyT[:, sl]

    def put_dx(c, sl, d):
        b.dxbuf[sl, :] = d.astype(BF16).T

    def step(s, carry):
        for gi in range(len(GROUPS)):
            if ISSUE[gi] > 0:
                @pl.when(s == ISSUE[gi])
                def _():
                    issue(gi)
        for j in range(N_CP):
            d = lax.rem(me + N_CP - j, N_CP)
            b.padrow[0:1, j * PIECE:(j + 1) * PIECE] = b.padin[d, pl.ds(s, 1), :]
        masks(b, b.padrow[0:1, :])
        for c in fetches(0, s):
            c.wait()
        b.xT[0] = b.xbuf[...].T
        forward(0, b, keep)
        for gi in range(len(GROUPS)):
            @pl.when(s == GROUPS[gi][0])
            def _():
                arrived(1, gi)
        for c in fetches(1, s):
            c.start()

        @pl.when(s > 0)
        def _():
            drain_out(0, s)
        forward(1, b, put_y)
        send_out(0, s)
        for c in fetches(1, s):
            c.wait()
        backward(1, b, get_dout, put_d)
        for gi in range(1, len(GROUPS)):
            @pl.when(s + 1 == GROUPS[gi][0])
            def _():
                arrived(0, gi)

        @pl.when(s + 1 < PER)
        def _():
            for c in fetches(0, s + 1):
                c.start()

        @pl.when(s > 0)
        def _():
            drain_out(1, s)
        backward(0, b, get_d, put_dx)
        send_out(1, s)
        return carry
    lax.fori_loop(0, PER, step, 0)

    for l in range(2):
        for k in range(2):
            b.dgs[l, k:k + 1, :] = jnp.sum(b.dg[k, l].T, axis=0, keepdims=True)
        b.dgs[l, 2:, :] = jnp.zeros((14, DIM), F32)
    for i, j in enumerate((mate, across)):
        pl.semaphore_signal(b.ready.at[i], inc=1, device_id={'cp': j}, device_id_type=pl.DeviceIdType.MESH)

    grads = {'aqkv': oqkv, 'aout': oout, 'ain': oin, 'adown': odown}

    def tile(ref, i, n):
        return ref.at[i // 6 if ref is b.mixT else i // 4,
                      pl.ds((i % 6 // 2 if ref is b.mixT else i % 4 // 2) * DIM, n), pl.ds(i % 2 * DIM, DIM)]

    def places(i):
        if i == len(BLOCKS):
            return (lambda l: b.dgs.at[l]), b.dgl, b.dgb, b.dgr, (lambda l: odg.at[l])
        name, r0, n, c0 = BLOCKS[i]
        acc, out = getattr(b, name), grads[name]
        return ((lambda l: acc.at[l, pl.ds(r0, n), pl.ds(c0, DIM)]), tile(b.mixT, i, n), tile(b.p1, i, n),
                tile(b.p1, i + 12, n), (lambda l: out.at[l, pl.ds(r0, n), pl.ds(c0, DIM)]))

    n_g = len(BLOCKS) + 1

    def first(i):
        acc, land, _, _, _ = places(i)
        return remote(acc(1 - core), land, b.g_send.at[0, i], b.g_recv.at[0, i], mate)

    def second(i):
        _, _, out, land, _ = places(i)
        return remote(out, land, b.g_send.at[1, i], b.g_recv.at[1, i], across)

    def third(i):
        acc, _, _, _, out = places(i)
        return (remote(acc(core), out(core), b.g_send.at[2, i], b.g_recv.at[2, i], mate),
                pltpu.make_async_copy(acc(core), out(core), b.g_own.at[i]))

    pl.semaphore_wait(b.ready.at[0], 1)
    for i in range(n_g):
        first(i).start()
    pl.semaphore_wait(b.ready.at[1], 1)
    for i in range(n_g):
        acc, land, out, _, _ = places(i)
        first(i).wait_recv()
        out[...] = (acc(core)[...] + land[...]).astype(BF16)
        second(i).start()
    for i in range(n_g):
        acc, _, mine, land, _ = places(i)
        second(i).wait_recv()
        acc(core)[...] = mine[...].astype(F32) + land[...].astype(F32)
        for c in third(i):
            c.start()
    for i in range(n_g):
        first(i).wait_send()
        second(i).wait_send()
        third(i)[0].wait()
        third(i)[1].wait()
    for c in pad_copies():
        c.wait_send()
    for a in range(2):
        drain_out(a, PER - 1)
        src = ins[a][0]
        buf, out = outs[a]
        for d in (1, 2, 3):
            whole_in = src.at[pl.ds(far(d) * PER, PER)]
            remote(whole_in, whole_in, b.in_send.at[a, d - 1], b.in_send.at[a, d - 1], far(d)).wait_send()
            whole_out = out.at[pl.ds(near(d) * PER, PER)]
            remote(whole_out, whole_out, b.out_recv.at[a, d - 1], b.out_recv.at[a, d - 1], near(d)).wait_recv()


def run_kernel(x, dout, pad, g, rope, w_qkv, w_out, w_in, w_down):
    any_spec = pl.BlockSpec(memory_space=pl.ANY)
    vm = pl.BlockSpec(memory_space=pltpu.VMEM)
    sds = jax.ShapeDtypeStruct
    outs = [sds(x.shape, BF16)] * 2 + [
        sds(s, F32) for s in ((2, DIM, 3 * DIM), (2, DIM, DIM), (2, DIM, 2 * FFN), (2, FFN, DIM), (2, 16, DIM))] + [
        sds((3, PER, PIECE, DIM), BF16)] * 2
    return pl.pallas_call(
        kernel, out_shape=outs,
        in_specs=[any_spec] * 3 + [vm] * 6,
        out_specs=[any_spec] * 9,
        scratch_shapes=scratch(),
        compiler_params=pltpu.CompilerParams(vmem_limit_bytes=67043328, collective_id=0, has_side_effects=True),
    )(x, dout, pad, g, rope, w_qkv, w_out, w_in, w_down)


def solution(mesh):
    act_spec = P('dp', 'cp', None)

    def device_pass(x_loc, pad_loc, dout_loc, g_attn, g_mlp, w_qkv, w_out, w_in, w_down):
        g = jnp.broadcast_to(jnp.stack([g_attn, g_mlp]).astype(F32)[..., None], (2, 2, DIM, 128))
        y, dx, dqkv, dout_w, din, ddown, dg = run_kernel(
            x_loc, dout_loc, pad_loc, g, jnp.asarray(rope_tables()), w_qkv, w_out, w_in, w_down)[:7]
        return y, dx, dg[:, 0], dg[:, 1], dqkv, dout_w, din, ddown

    return jax.shard_map(device_pass, mesh=mesh,
                         in_specs=(act_spec, P('dp', 'cp'), act_spec, P(), P(), P(), P(), P(), P()),
                         out_specs=(act_spec, act_spec, P('dp'), P('dp'), P('dp'), P('dp'), P('dp'), P('dp')),
                         check_vma=False)
```

```python
import numpy as np
import jax
import jax.numpy as jnp
from jax import lax
from jax.experimental import pallas as pl
from jax.experimental.pallas import tpu as pltpu
from jax.sharding import PartitionSpec as P

HEADS = 6
HD = 64
WIN = 64
EPS = 1e-5
THETAS = (10000.0, 160000.0)
NEG = -1e30
SEQ = 768
DIM = 384
FFN = 576
CH = 256
NCH = SEQ // CH
F32 = jnp.float32
BF16 = jnp.bfloat16
KEYS = (((0, 384), (128, 640), (384, 768)), ((0, 768),) * 3)


def rope_tables():
    out = np.zeros((2, 2, HD // 2, SEQ), np.float32)
    pos = np.arange(SEQ, dtype=np.float32)
    for l, theta in enumerate(THETAS):
        freq = np.float32(theta) ** (-np.arange(0, HD, 2, dtype=np.float32) / np.float32(HD))
        ang = (pos[None, :] * freq.astype(np.float32)[:, None]).astype(np.float32).astype(np.float64)
        out[l, 0] = np.cos(ang)
        out[l, 1] = np.sin(ang)
    return out


def nn(a, b):
    return jnp.dot(a, b, preferred_element_type=F32)


def nt(a, b):
    return lax.dot_general(a, b, (((1,), (1,)), ((), ())), preferred_element_type=F32)


def wide(g):
    return jnp.concatenate([g] * (CH // 128), axis=1)


def fold(z):
    return sum(z[:, i * 128:(i + 1) * 128] for i in range(1, CH // 128)) + z[:, :128]


def ln_fwd(z, gain, st, row, sl):
    mean = jnp.sum(z, axis=0, keepdims=True) * (1.0 / DIM)
    c = z - mean
    var = jnp.sum(c * c, axis=0, keepdims=True) * (1.0 / DIM)
    r = lax.rsqrt(var + EPS)
    st[row:row + 1, sl] = mean
    st[row + 1:row + 2, sl] = r
    return (c * r * wide(gain)).astype(BF16)


def ln_bwd(z, du, gain, st, row, sl):
    mean = st[row:row + 1, sl]
    r = st[row + 1:row + 2, sl]
    xhat = (z - mean) * r
    dg = fold(du * xhat)
    gw = wide(gain)
    dxh = du * gw
    m1 = jnp.sum(dxh, axis=0, keepdims=True) * (1.0 / DIM)
    m2 = jnp.sum(dxh * xhat, axis=0, keepdims=True) * (1.0 / DIM)
    return r * (dxh - m1 - xhat * m2), dg, (xhat * gw).astype(BF16)


def turn(z, cos, sin):
    n = z.shape[0] // HD
    z4 = z.reshape(n, 2, HD // 2, z.shape[1])
    a, b = z4[:, 0], z4[:, 1]
    return jnp.stack([a * cos - b * sin, b * cos + a * sin], axis=1).reshape(z.shape)


def gelu_parts(a):
    cdf = 0.5 * (1.0 + lax.erf(a * (2.0 ** -0.5)))
    return a * cdf, cdf


class Bufs:
    pass


def forward(l, b, write_y):
    st = b.st.at[l]
    tmp = {}

    def norm_in(c):
        sl = pl.ds(c * CH, CH)
        tmp['z', c] = nn(b.wTqkv[l], ln_fwd(b.xT[l, :, sl].astype(F32), b.g[0, l], st, 0, sl))

    def rotate(c):
        sl = pl.ds(c * CH, CH)
        z = tmp.pop(('z', c))
        cos, sin = b.rope[l, 0, :, sl], b.rope[l, 1, :, sl]
        b.qkvT[l, :DIM, sl] = turn(z[:DIM], cos * 0.125, sin * 0.125).astype(BF16)
        b.qkvT[l, DIM:2 * DIM, sl] = turn(z[DIM:2 * DIM], cos, sin).astype(BF16)
        b.qkvT[l, 2 * DIM:, sl] = z[2 * DIM:].astype(BF16)

    norm_in(0)
    norm_in(1)
    rotate(0)
    norm_in(2)
    rotate(1)
    rotate(2)

    def group(i, carry):
        heads = [3 * i, 3 * i + 1, 3 * i + 2]
        rows_of = [pl.multiple_of(h * HD, HD) for h in heads]
        keys = []
        for row in rows_of:
            kT = b.qkvT[l, pl.ds(DIM + row, HD), :]
            keys.append(kT.T if l == 0 else jnp.concatenate([kT, b.kextra[...]], axis=0).T)

        def score(n):
            k, c = divmod(n, NCH)
            k0, k1 = KEYS[l][c]
            qT = b.qkvT[l, pl.ds(rows_of[k], HD), pl.ds(c * CH, CH)]
            if l == 0:
                return nn(keys[k][k0:k1], qT) + b.bias[c, :k1 - k0, :].astype(F32)
            return nn(keys[k], jnp.concatenate([qT, b.qextra[...]], axis=0))

        total = len(heads) * NCH
        s = score(0)
        for n in range(total):
            k, c = divmod(n, NCH)
            sl = pl.ds(c * CH, CH)
            k0, k1 = KEYS[l][c]
            later = score(n + 1) if n + 1 < total else None
            m = jnp.max(s, axis=0, keepdims=True)
            e = jnp.exp(s - m)
            p = (e * (1.0 / jnp.sum(e, axis=0, keepdims=True))).astype(BF16)
            if l == 0:
                b.p0[heads[k], c, :k1 - k0, :] = p
            else:
                b.p1[heads[k], :, sl] = p
            vT = b.qkvT[l, pl.ds(2 * DIM + rows_of[k], HD), k0:k1]
            b.oT[l, pl.ds(rows_of[k], HD), sl] = nn(vT, p).astype(BF16)
            s = later
        return carry
    lax.fori_loop(0, HEADS // 3, group, 0)

    def open_mlp(c):
        sl = pl.ds(c * CH, CH)
        hb = (b.xT[l, :, sl].astype(F32) + nn(b.wTout[l], b.oT[l, :, sl])).astype(BF16)
        b.hT[l, :, sl] = hb
        b.mixT[l, :, sl] = nn(b.wTin[l], ln_fwd(hb.astype(F32), b.g[1, l], st, 2, sl))

    def close_mlp(c):
        sl = pl.ds(c * CH, CH)
        act = (gelu_parts(b.mixT[l, :FFN, sl])[0] * b.mixT[l, FFN:, sl]).astype(BF16)
        write_y(c, sl, (b.hT[l, :, sl].astype(F32) + nn(b.wTdown[l], act)).astype(BF16))

    open_mlp(0)
    open_mlp(1)
    close_mlp(0)
    open_mlp(2)
    close_mlp(1)
    close_mlp(2)


def backward(l, b, read_dy, write_dx):
    st = b.st.at[l]
    tmp = {}

    def gate(c):
        sl = pl.ds(c * CH, CH)
        dyb = read_dy(c, sl).astype(BF16)
        b.dybT[:, sl] = dyb
        tmp['act', c] = nn(b.wdown[l], dyb)

    def ungate(c):
        sl = pl.ds(c * CH, CH)
        dact = tmp.pop(('act', c))
        a, g = b.mixT[l, :FFN, sl], b.mixT[l, FFN:, sl]
        ge, cdf = gelu_parts(a)
        b.actT[:, sl] = (ge * g).astype(BF16)
        pdf = jnp.exp(a * a * -0.5) * 0.3989422804014327
        b.dbigT[:FFN, sl] = (dact * g * (cdf + a * pdf)).astype(BF16)
        b.dbigT[FFN:, sl] = (dact * ge).astype(BF16)
        tmp['du', c] = nn(b.win[l], b.dbigT[:, sl])

    def unnorm(c):
        sl = pl.ds(c * CH, CH)
        dn, dg, b.uT[:, sl] = ln_bwd(b.hT[l, :, sl].astype(F32), tmp.pop(('du', c)), b.g[1, l], st, 2, sl)
        b.dg[1, l] += dg
        dh = read_dy(c, sl) + dn
        b.dyT[:, sl] = dh
        dhb = dh.astype(BF16)
        b.dhbT[:, sl] = dhb
        b.doT[:, sl] = nn(b.wout[l], dhb).astype(BF16)

    gate(0)
    gate(1)
    ungate(0)
    gate(2)
    ungate(1)
    unnorm(0)
    ungate(2)
    unnorm(1)
    b.adown[l] += nt(b.actT[...], b.dybT[...])
    unnorm(2)
    b.ain[l] += nt(b.uT[...], b.dbigT[...])
    b.aout[l] += nt(b.oT[l], b.dhbT[...])

    def group(i, carry):
        heads = [3 * i, 3 * i + 1, 3 * i + 2]
        info = []
        for h in heads:
            row = pl.multiple_of(h * HD, HD)
            doT = b.doT[pl.ds(row, HD), :]
            prod = doT.astype(F32) * b.oT[l, pl.ds(row, HD), :].astype(F32)
            info.append((h, row, b.qkvT[l, pl.ds(row, HD), :], b.qkvT[l, pl.ds(DIM + row, HD), :],
                         b.qkvT[l, pl.ds(2 * DIM + row, HD), :].T, doT, jnp.sum(prod, axis=0, keepdims=True)))

        def dprob(n):
            k, c = divmod(n, NCH)
            k0, k1 = KEYS[l][c]
            return nn(info[k][4][k0:k1], info[k][5][:, c * CH:(c + 1) * CH])

        cos, sin = b.rope[l, 0], -b.rope[l, 1]
        total = len(heads) * NCH
        dp = dprob(0)
        for n in range(total):
            k, c = divmod(n, NCH)
            h, row, qT, kT, _, doT, delta = info[k]
            if c == 0:
                dq, dk, dv = [], [None] * 6, [None] * 6
            cs = slice(c * CH, (c + 1) * CH)
            sl = pl.ds(c * CH, CH)
            k0, k1 = KEYS[l][c]
            later = dprob(n + 1) if n + 1 < total else None
            p = b.p0[h, c, :k1 - k0, :] if l == 0 else b.p1[h, :, sl]
            ds = (p.astype(F32) * (dp - delta[:, cs])).astype(BF16)
            dp = later
            dq.append(nn(kT[:, k0:k1], ds) * 0.125)
            dkc, dvc = nt(qT[:, cs], ds), nt(doT[:, cs], p)
            for j in range(k0 // 128, k1 // 128):
                js = slice(j * 128 - k0, (j + 1) * 128 - k0)
                dk[j] = dkc[:, js] if dk[j] is None else dk[j] + dkc[:, js]
                dv[j] = dvc[:, js] if dv[j] is None else dv[j] + dvc[:, js]
            if c < NCH - 1:
                continue
            dkT, dvT = jnp.concatenate(dk, axis=1), jnp.concatenate(dv, axis=1)
            b.dbigT[pl.ds(row, HD), :] = turn(jnp.concatenate(dq, axis=1), cos, sin).astype(BF16)
            b.dbigT[pl.ds(DIM + row, HD), :] = turn(dkT, cos, sin).astype(BF16)
            b.dbigT[pl.ds(2 * DIM + row, HD), :] = dvT.astype(BF16)
        return carry
    lax.fori_loop(0, HEADS // 3, group, 0)

    def unproject(c):
        tmp['du', c] = nn(b.wqkv[l], b.dbigT[:, pl.ds(c * CH, CH)])

    def finish(c):
        sl = pl.ds(c * CH, CH)
        dn, dg, b.uT[:, sl] = ln_bwd(b.xT[l, :, sl].astype(F32), tmp.pop(('du', c)), b.g[0, l], st, 0, sl)
        b.dg[0, l] += dg
        write_dx(c, sl, b.dyT[:, sl] + dn)

    unproject(0)
    unproject(1)
    finish(0)
    unproject(2)
    finish(1)
    finish(2)
    b.aqkv[l] += nt(b.uT[...], b.dbigT[...])


def start_up(b):
    for src, dst in ((b.wqkv, b.wTqkv), (b.wout, b.wTout), (b.win, b.wTin), (b.wdown, b.wTdown)):
        for l in range(2):
            dst[l] = src[l].T
    for acc in (b.aqkv, b.aout, b.ain, b.adown, b.dg):
        acc[...] = jnp.zeros_like(acc)
    row0 = lax.broadcasted_iota(jnp.int32, (HD, CH), 0) == 0
    b.qextra[...] = jnp.where(row0, 1.0, 0.0).astype(BF16)


def masks(b, pad):
    ok = pad > 0
    row0 = lax.broadcasted_iota(jnp.int32, (HD, SEQ), 0) == 0
    b.kextra[...] = jnp.where(row0 & jnp.logical_not(ok), NEG, 0.0).astype(BF16)
    okc = jnp.broadcast_to(jnp.where(ok, 1.0, 0.0), (128, SEQ)).T
    for c in range(NCH):
        k0, k1 = KEYS[0][c]
        shape = (k1 - k0, CH)
        off = lax.broadcasted_iota(jnp.int32, shape, 0) + (k0 - c * CH) - lax.broadcasted_iota(jnp.int32, shape, 1)
        near = (jnp.abs(off) <= WIN) & (wide(okc[k0:k1]) > 0.5)
        b.bias[c, :k1 - k0, :] = jnp.where(near | (off == 0), 0.0, NEG).astype(BF16)


NAMES = ('wTqkv', 'wTout', 'wTin', 'wTdown', 'aqkv', 'aout', 'ain', 'adown', 'dg', 'st', 'xT', 'uT', 'qkvT',
         'p0', 'p1', 'oT', 'hT', 'mixT', 'actT', 'dyT', 'dybT', 'dbigT', 'dhbT', 'doT', 'bias',
         'kextra', 'qextra', 'xbuf', 'dbuf', 'ybuf', 'dxbuf', 'padin', 'padrow', 'dgs', 'dgl', 'dgb', 'dgr',
         'in_send', 'in_recv', 'pad_send', 'pad_recv', 'fetch', 'out_send', 'out_recv', 'own', 'ready',
         'g_send', 'g_recv', 'g_own')

N_CP = 4
PER = 8
PIECE = SEQ // N_CP
GROUPS = ((0, 1), (1, 1), (2, 2), (4, 4))
ISSUE = (0, 0, 1, 2)
BLOCKS = tuple([('aqkv', 0, DIM, i * DIM) for i in range(3)] + [('ain', 0, DIM, i * DIM) for i in range(3)]
               + [('aout', 0, DIM, 0), ('adown', 0, DIM, 0), ('adown', DIM, FFN - DIM, 0)])


def scratch():
    v = pltpu.VMEM
    dma, reg = pltpu.SemaphoreType.DMA, pltpu.SemaphoreType.REGULAR
    n_g = len(BLOCKS) + 1
    return [v((2, 3 * DIM, DIM), BF16), v((2, DIM, DIM), BF16), v((2, 2 * FFN, DIM), BF16), v((2, DIM, FFN), BF16),
            v((2, DIM, 3 * DIM), F32), v((2, DIM, DIM), F32), v((2, DIM, 2 * FFN), F32), v((2, FFN, DIM), F32),
            v((2, 2, DIM, 128), F32), v((2, 8, SEQ), F32),
            v((2, DIM, SEQ), BF16), v((DIM, SEQ), BF16), v((2, 3 * DIM, SEQ), BF16),
            v((HEADS, NCH, 512, CH), BF16), v((HEADS, SEQ, SEQ), BF16),
            v((2, DIM, SEQ), BF16), v((2, DIM, SEQ), BF16), v((2, 2 * FFN, SEQ), F32),
            v((FFN, SEQ), BF16), v((DIM, SEQ), F32), v((DIM, SEQ), BF16), v((3 * DIM, SEQ), BF16),
            v((DIM, SEQ), BF16), v((DIM, SEQ), BF16), v((NCH, 512, CH), BF16),
            v((HD, SEQ), BF16), v((HD, CH), BF16),
            v((SEQ, DIM), BF16), v((SEQ, DIM), BF16), v((SEQ, DIM), BF16), v((SEQ, DIM), BF16),
            v((N_CP, PER, PIECE), jnp.int32), v((8, SEQ), jnp.int32),
            v((2, 16, DIM), F32), v((16, DIM), F32), v((16, DIM), BF16), v((16, DIM), BF16),
            dma((2, 3)), dma((2, len(GROUPS), 3)), dma((3,)), dma((3,)), dma((3, N_CP)),
            dma((2, 3)), dma((2, 3)), dma((2,)), reg((2,)),
            dma((3, n_g)), dma((3, n_g)), dma((n_g,))]


def rows(j):
    return pl.ds(pl.multiple_of(j * PIECE, 64), PIECE)


def kernel(x_loc, dout_loc, pad_loc, g_ref, rope_ref, wqkv, wout, win, wdown,
           y_out, dx_out, oqkv, oout, oin, odown, odg, xland, dland, *refs):
    b = Bufs()
    for name, ref in zip(NAMES, refs):
        setattr(b, name, ref)
    b.g, b.rope, b.wqkv, b.wout, b.win, b.wdown = g_ref, rope_ref, wqkv, wout, win, wdown
    me = lax.axis_index('cp')
    core = lax.rem(me, 2)
    mate = me + 1 - 2 * core
    across = lax.rem(me + 2, N_CP)

    def far(d):
        return lax.rem(me + d, N_CP)

    def near(d):
        return lax.rem(me + N_CP - d, N_CP)

    def remote(src, dst, ssem, rsem, j):
        return pltpu.make_async_remote_copy(src_ref=src, dst_ref=dst, send_sem=ssem, recv_sem=rsem,
                                            device_id={'cp': j}, device_id_type=pl.DeviceIdType.MESH)

    ins = ((x_loc, xland), (dout_loc, dland))
    outs = ((b.ybuf, y_out), (b.dxbuf, dx_out))

    def send_in(a, gi, d):
        first, n = GROUPS[gi]
        src, land = ins[a]
        return remote(src.at[pl.ds(far(d) * PER + first, n)], land.at[d - 1, pl.ds(first, n)],
                      b.in_send.at[a, d - 1], b.in_recv.at[a, gi, d - 1], far(d))

    def issue(gi):
        for a in range(2):
            for d in (2, 1, 3):
                send_in(a, gi, d).start()

    def arrived(a, gi):
        for d in (1, 2, 3):
            send_in(a, gi, d).wait_recv()

    def fetches(a, s):
        src, land = ins[a]
        buf = (b.xbuf, b.dbuf)[a]
        res = [pltpu.make_async_copy(src.at[me * PER + s], buf.at[rows(me)], b.fetch.at[a, 0])]
        for d in (1, 2, 3):
            res.append(pltpu.make_async_copy(land.at[d - 1, s], buf.at[rows(near(d))], b.fetch.at[a, d]))
        return res

    def out_copies(a, s):
        buf, out = outs[a]
        res = [remote(buf.at[rows(far(d))], out.at[me * PER + s], b.out_send.at[a, d - 1], b.out_recv.at[a, d - 1], far(d))
               for d in (2, 1, 3)]
        return res, pltpu.make_async_copy(buf.at[rows(me)], out.at[me * PER + s], b.own.at[a])

    def send_out(a, s):
        res, own = out_copies(a, s)
        for c in res:
            c.start()
        own.start()

    def drain_out(a, s):
        res, own = out_copies(a, s)
        for c in res:
            c.wait_send()
        own.wait()

    def pad_copies():
        return [remote(pad_loc.at[pl.ds(pl.multiple_of(far(d) * PER, PER), PER)], b.padin.at[d], b.pad_send.at[d - 1],
                       b.pad_recv.at[d - 1], far(d)) for d in (1, 2, 3)]

    barrier = pltpu.get_barrier_semaphore()
    for d in (1, 2, 3):
        pl.semaphore_signal(barrier, inc=1, device_id={'cp': far(d)}, device_id_type=pl.DeviceIdType.MESH)
    pl.semaphore_wait(barrier, 3)
    for c in pad_copies():
        c.start()
    pad_own = pltpu.make_async_copy(pad_loc.at[pl.ds(pl.multiple_of(me * PER, PER), PER)], b.padin.at[0], b.fetch.at[2, 0])
    pad_own.start()
    for gi in range(len(GROUPS)):
        if ISSUE[gi] == 0:
            issue(gi)
    start_up(b)
    pad_own.wait()
    for c in pad_copies():
        c.wait_recv()
    arrived(0, 0)
    for c in fetches(0, 0):
        c.start()

    def keep(c, sl, y):
        b.xT[1, :, sl] = y

    def put_y(c, sl, y):
        b.ybuf[sl, :] = y.T

    def get_dout(c, sl):
        return b.dbuf[sl, :].T.astype(F32)

    def put_d(c, sl, d):
        b.dyT[:, sl] = d

    def get_d(c, sl):
        return b.dyT[:, sl]

    def put_dx(c, sl, d):
        b.dxbuf[sl, :] = d.astype(BF16).T

    def step(s, carry):
        for gi in range(len(GROUPS)):
            if ISSUE[gi] > 0:
                @pl.when(s == ISSUE[gi])
                def _():
                    issue(gi)
        for j in range(N_CP):
            d = lax.rem(me + N_CP - j, N_CP)
            b.padrow[0:1, j * PIECE:(j + 1) * PIECE] = b.padin[d, pl.ds(s, 1), :]
        masks(b, b.padrow[0:1, :])
        for c in fetches(0, s):
            c.wait()
        b.xT[0] = b.xbuf[...].T
        forward(0, b, keep)
        for gi in range(len(GROUPS)):
            @pl.when(s == GROUPS[gi][0])
            def _():
                arrived(1, gi)
        for c in fetches(1, s):
            c.start()

        @pl.when(s > 0)
        def _():
            drain_out(0, s)
        forward(1, b, put_y)
        send_out(0, s)
        for c in fetches(1, s):
            c.wait()
        backward(1, b, get_dout, put_d)
        for gi in range(1, len(GROUPS)):
            @pl.when(s + 1 == GROUPS[gi][0])
            def _():
                arrived(0, gi)

        @pl.when(s + 1 < PER)
        def _():
            for c in fetches(0, s + 1):
                c.start()

        @pl.when(s > 0)
        def _():
            drain_out(1, s)
        backward(0, b, get_d, put_dx)
        send_out(1, s)
        return carry
    lax.fori_loop(0, PER, step, 0)

    for l in range(2):
        for k in range(2):
            b.dgs[l, k:k + 1, :] = jnp.sum(b.dg[k, l].T, axis=0, keepdims=True)
        b.dgs[l, 2:, :] = jnp.zeros((14, DIM), F32)
    for i, j in enumerate((mate, across)):
        pl.semaphore_signal(b.ready.at[i], inc=1, device_id={'cp': j}, device_id_type=pl.DeviceIdType.MESH)

    grads = {'aqkv': oqkv, 'aout': oout, 'ain': oin, 'adown': odown}

    def tile(ref, i, n):
        return ref.at[i // 6 if ref is b.mixT else i // 4,
                      pl.ds((i % 6 // 2 if ref is b.mixT else i % 4 // 2) * DIM, n), pl.ds(i % 2 * DIM, DIM)]

    def places(i):
        if i == len(BLOCKS):
            return (lambda l: b.dgs.at[l]), b.dgl, b.dgb, b.dgr, (lambda l: odg.at[l])
        name, r0, n, c0 = BLOCKS[i]
        acc, out = getattr(b, name), grads[name]
        return ((lambda l: acc.at[l, pl.ds(r0, n), pl.ds(c0, DIM)]), tile(b.mixT, i, n), tile(b.p1, i, n),
                tile(b.p1, i + 12, n), (lambda l: out.at[l, pl.ds(r0, n), pl.ds(c0, DIM)]))

    n_g = len(BLOCKS) + 1

    def first(i):
        acc, land, _, _, _ = places(i)
        return remote(acc(1 - core), land, b.g_send.at[0, i], b.g_recv.at[0, i], mate)

    def second(i):
        _, _, out, land, _ = places(i)
        return remote(out, land, b.g_send.at[1, i], b.g_recv.at[1, i], across)

    def third(i):
        acc, _, _, _, out = places(i)
        return (remote(acc(core), out(core), b.g_send.at[2, i], b.g_recv.at[2, i], mate),
                pltpu.make_async_copy(acc(core), out(core), b.g_own.at[i]))

    pl.semaphore_wait(b.ready.at[0], 1)
    for i in range(n_g):
        first(i).start()
    pl.semaphore_wait(b.ready.at[1], 1)
    for i in range(n_g):
        acc, land, out, _, _ = places(i)
        first(i).wait_recv()
        out[...] = (acc(core)[...] + land[...]).astype(BF16)
        second(i).start()
    for i in range(n_g):
        acc, _, mine, land, _ = places(i)
        second(i).wait_recv()
        acc(core)[...] = mine[...].astype(F32) + land[...].astype(F32)
        for c in third(i):
            c.start()
    for i in range(n_g):
        first(i).wait_send()
        second(i).wait_send()
        third(i)[0].wait()
        third(i)[1].wait()
    for c in pad_copies():
        c.wait_send()
    for a in range(2):
        drain_out(a, PER - 1)
        src = ins[a][0]
        buf, out = outs[a]
        for d in (1, 2, 3):
            whole_in = src.at[pl.ds(far(d) * PER, PER)]
            remote(whole_in, whole_in, b.in_send.at[a, d - 1], b.in_send.at[a, d - 1], far(d)).wait_send()
            whole_out = out.at[pl.ds(near(d) * PER, PER)]
            remote(whole_out, whole_out, b.out_recv.at[a, d - 1], b.out_recv.at[a, d - 1], near(d)).wait_recv()


def run_kernel(x, dout, pad, g, rope, w_qkv, w_out, w_in, w_down):
    any_spec = pl.BlockSpec(memory_space=pl.ANY)
    vm = pl.BlockSpec(memory_space=pltpu.VMEM)
    sds = jax.ShapeDtypeStruct
    outs = [sds(x.shape, BF16)] * 2 + [
        sds(s, F32) for s in ((2, DIM, 3 * DIM), (2, DIM, DIM), (2, DIM, 2 * FFN), (2, FFN, DIM), (2, 16, DIM))] + [
        sds((3, PER, PIECE, DIM), BF16)] * 2
    return pl.pallas_call(
        kernel, out_shape=outs,
        in_specs=[any_spec] * 3 + [vm] * 6,
        out_specs=[any_spec] * 9,
        scratch_shapes=scratch(),
        compiler_params=pltpu.CompilerParams(vmem_limit_bytes=67043328, collective_id=0, has_side_effects=True),
    )(x, dout, pad, g, rope, w_qkv, w_out, w_in, w_down)


def solution(mesh):
    act_spec = P('dp', 'cp', None)

    def device_pass(x_loc, pad_loc, dout_loc, g_attn, g_mlp, w_qkv, w_out, w_in, w_down):
        g = jnp.broadcast_to(jnp.stack([g_attn, g_mlp]).astype(F32)[..., None], (2, 2, DIM, 128))
        y, dx, dqkv, dout_w, din, ddown, dg = run_kernel(
            x_loc, dout_loc, pad_loc, g, jnp.asarray(rope_tables()), w_qkv, w_out, w_in, w_down)[:7]
        return y, dx, dg[:, 0], dg[:, 1], dqkv, dout_w, din, ddown

    return jax.shard_map(device_pass, mesh=mesh,
                         in_specs=(act_spec, P('dp', 'cp'), act_spec, P(), P(), P(), P(), P(), P()),
                         out_specs=(act_spec, act_spec, P('dp'), P('dp'), P('dp'), P('dp'), P('dp'), P('dp')),
                         check_vma=False)
```
